256 devices in a mesh: dom: 256 (over z, x, y, core).
Axes of the slice: x: 4, y: 4, z: 8, core: 2. Of those that a mesh axis runs over, the one named last changes fastest.
Arguments:
- entities: float32 [262144, 200], P('dom'), may hold values from -3 to 3
- entity_state: float32 [262144], P('dom'), may hold values from 1e-05 to 0.1
- relations: float32 [1345, 200], replicated, may hold values from -3 to 3
- relation_state: float32 [1345], replicated, may hold values from 1 to 100
- edges: int32 [2, 3, 131072], P(None, None, 'dom'), may hold values from 0 to 1344, as said below
- negatives: int32 [2, 1024, 1000], P(None, 'dom'), may hold values from 0 to 1023
- counts: int32 [2, 256], P(None, 'dom'), may hold values from 1 to 512, as said below
Outputs:
- entities_after: float32 [262144, 200], P('dom')
- entity_state_after: float32 [262144], P('dom')
- relations_after: float32 [1345, 200], replicated
- relation_state_after: float32 [1345], replicated
The draws below stay inside these ranges and needn't reach their ends.
Inputs may be any that keep to these rules, and one draw needn't show every extreme that they name: `edges`: rows 0 and 2 are local entity ids below 1024; row 1 holds relation ids below 1345. `negatives`: local ids in the partner's partition. `counts`: in every round some bucket is full.
All inputs are finite; a program needn't handle non-finite values.
Results may differ from the reference program's by a relative error of at most 0.0003.
Values sent between devices are 32-bit elements; how exact they have to be, the bound alone decides.
A program may use at most 64 MiB of HBM per device.

```python
import math
import jax
import jax.numpy as jnp
from jax import lax

ENT_DEV = 1024
DIM = 200
REL = 1345
NEG = 1000
BLOCK = 128
BLOCKS = 4
ROUNDS = 2
EDGES_DEV = 512
PARTITIONS = 256
ENTITIES = 262144
TOTAL_EDGES = 131072
ALL_BLOCKS = 1024


def draw_edges(key, part):
    keys = jax.random.split(jax.random.fold_in(key, 11), 4)
    source = jax.random.randint(keys[0], (ROUNDS, 1, TOTAL_EDGES), 0, ENT_DEV, dtype=jnp.int32)
    target = jax.random.randint(keys[1], (ROUNDS, 1, TOTAL_EDGES), 0, ENT_DEV, dtype=jnp.int32)
    first = jax.random.randint(keys[2], (ROUNDS, 1, TOTAL_EDGES), 0, REL, dtype=jnp.int32)
    second = jax.random.randint(keys[3], (ROUNDS, 1, TOTAL_EDGES), 0, REL, dtype=jnp.int32)
    relation = first * second // REL
    return jnp.concatenate([source, relation, target], axis=1).astype(jnp.int32)


def draw_counts(key, part):
    keys = jax.random.split(jax.random.fold_in(key, 23), 3)
    first = jax.random.randint(keys[0], (ROUNDS, PARTITIONS), 0, EDGES_DEV, dtype=jnp.int32)
    second = jax.random.randint(keys[1], (ROUNDS, PARTITIONS), 0, EDGES_DEV, dtype=jnp.int32)
    filled = 1 + first * second // EDGES_DEV
    fullest = jax.random.randint(keys[2], (ROUNDS, 1), 0, PARTITIONS, dtype=jnp.int32)
    places = jnp.arange(PARTITIONS, dtype=jnp.int32)[None, :]
    return jnp.where(places == fullest, EDGES_DEV, filled).astype(jnp.int32)


def set_ends(values, rng, smallest, high):
    extent = values.shape
    place = [jax.random.randint(jax.random.fold_in(rng, axis), (), 0, extent[axis]) for axis in range(len(extent))]
    values = values.at[tuple(place)].set(smallest)
    longest = extent.index(max(extent))
    place[longest] = (place[longest] + 1) % extent[longest]
    return values.at[tuple(place)].set(high)


def shard_levels(key, extent, cuts, smallest, high):
    def one(dim, parts):
        heights = jax.random.uniform(jax.random.fold_in(jax.random.fold_in(key, 6), dim), (parts,), jnp.float32, smallest / len(cuts), high / len(cuts))
        return jnp.repeat(jnp.exp(heights), extent[dim] // parts).reshape((-1,) + (1,) * (len(extent) - dim - 1))

    loudness = one(*cuts[0])
    for cut in cuts[1:]:
        loudness = loudness * one(*cut)
    return loudness


def scatter_about(stream_key, dims, scale, bound, shards=(), kind=jnp.bfloat16):
    drawn = scale * jax.random.normal(stream_key, dims, jnp.float32)
    if shards:
        drawn = drawn * shard_levels(stream_key, dims, shards, -0.22, 0.18)
    return jnp.clip(drawn, -bound, bound).astype(kind)


def setup_inputs(seed: int = 0) -> dict:
    seeds = jax.random.split(jax.random.key(seed), 8)
    return {
        "entities": scatter_about(seeds[0], (ENTITIES, DIM), 0.5, 3.0, ((0, 256),), jnp.float32),
        "entity_state": jnp.clip(jnp.exp(math.log(0.1) - 9.2103404 * jax.random.uniform(seeds[1], (ENTITIES,), jnp.float32) ** shard_levels(seeds[1], (ENTITIES,), ((0, 256),), -0.2, 0.2)), 9.999999747378752e-06, 0.1),
        "relations": scatter_about(seeds[2], (REL, DIM), 0.5, 3.0, (), jnp.float32),
        "relation_state": jnp.clip(jnp.exp(jax.random.uniform(seeds[3], (REL,), jnp.float32, math.log(1.0), math.log(100.0))), 1.0, 100.0),
        "edges": draw_edges(jax.random.fold_in(seeds[7], 71), 0),
        "negatives": set_ends(jax.random.randint(seeds[5], (ROUNDS, ALL_BLOCKS, NEG), 0, ENT_DEV), jax.random.fold_in(seeds[5], 1), 0, ENT_DEV - 1).astype(jnp.int32),
        "counts": draw_counts(jax.random.fold_in(seeds[7], 71), 0),
    }


RATE = 0.2
HIGH = lax.Precision.HIGHEST

def block_terms(carry, table, relations, source, relation, target, negative_ids, live):
    grad_table, grad_relation = carry
    half = table.shape[1] // 2
    src_rows = table[source]
    tgt_rows = table[target]
    neg_rows = table[negative_ids]
    rel_rows = relations[relation]
    src_real, src_imag = (src_rows[:, :half], src_rows[:, half:])
    rel_real, rel_imag = (rel_rows[:, :half], rel_rows[:, half:])
    product = jnp.concatenate([src_real * rel_real - src_imag * rel_imag, src_real * rel_imag + src_imag * rel_real], axis=1)
    positive = lax.optimization_barrier(jnp.sum(product * tgt_rows, axis=1))
    negative = lax.dot_general(product, neg_rows, (((1,), (1,)), ((), ())), precision=HIGH, preferred_element_type=jnp.float32)
    pos_weight = -jax.nn.sigmoid(-positive) * live
    neg_weight = jax.nn.sigmoid(negative) * (live[:, None] / negative.shape[1])
    upstream = pos_weight[:, None] * tgt_rows + jnp.dot(neg_weight, neg_rows, precision=HIGH, preferred_element_type=jnp.float32)
    target_grad = pos_weight[:, None] * product
    negative_grad = lax.dot_general(neg_weight, product, (((0,), (0,)), ((), ())), precision=HIGH, preferred_element_type=jnp.float32)
    up_real, up_imag = (upstream[:, :half], upstream[:, half:])
    source_grad = jnp.concatenate([up_real * rel_real + up_imag * rel_imag, up_imag * rel_real - up_real * rel_imag], axis=1)
    relation_grad = jnp.concatenate([up_real * src_real + up_imag * src_imag, up_imag * src_real - up_real * src_imag], axis=1)
    grad_table = grad_table.at[source].add(source_grad).at[target].add(target_grad).at[negative_ids].add(negative_grad)
    grad_relation = grad_relation.at[relation].add(relation_grad)
    return (grad_table, grad_relation)

def bucket_pass(carry, table, relations, edge_pair, negative_pair, count_pair, source_shift, target_shift, block, first, last):
    block_pair = (count_pair + block - 1) // block

    def visit(index, inner):
        which = (index >= block_pair[0]).astype(jnp.int32)
        number = (index - which * block_pair[0]).astype(jnp.int32)
        edge_list = lax.dynamic_index_in_dim(edge_pair, which, 0, keepdims=False)
        start = (number * block).astype(jnp.int32)
        window = lax.dynamic_slice_in_dim(edge_list, start, block, 1)
        negative_list = lax.dynamic_index_in_dim(negative_pair, which, 0, keepdims=False)
        negative_ids = lax.dynamic_index_in_dim(negative_list, number, 0, keepdims=False) + target_shift[which]
        live = (start + jnp.arange(block, dtype=jnp.int32) < count_pair[which]).astype(jnp.float32)
        return block_terms(inner, table, relations, window[0] + source_shift[which], window[1], window[2] + target_shift[which], negative_ids, live)
    return lax.fori_loop(first, last, visit, carry)

def adagrad(param, state, grad):
    new_state = state + lax.optimization_barrier(jnp.mean(grad * grad, axis=1))
    return (param - RATE * grad / jnp.sqrt(new_state)[:, None], new_state)

def round_pass(entities, entity_state, relations, edge_round, negative_round, count_round, span):
    source_shift = jnp.array([0, ENT_DEV], dtype=jnp.int32)
    target_shift = jnp.array([ENT_DEV, 0], dtype=jnp.int32)

    def visit_pair(pair, carry):
        new_entities, new_state, grad_relation = carry
        pair = pair.astype(jnp.int32)
        lower = (pair // span * (2 * span) + pair % span).astype(jnp.int32)
        upper = (lower + span).astype(jnp.int32)
        low_rows = lax.dynamic_slice_in_dim(entities, (lower * ENT_DEV).astype(jnp.int32), ENT_DEV, 0)
        high_rows = lax.dynamic_slice_in_dim(entities, (upper * ENT_DEV).astype(jnp.int32), ENT_DEV, 0)
        table = jnp.concatenate([low_rows, high_rows], axis=0)
        edge_pair = jnp.stack([lax.dynamic_slice_in_dim(edge_round, (lower * EDGES_DEV).astype(jnp.int32), EDGES_DEV, 1), lax.dynamic_slice_in_dim(edge_round, (upper * EDGES_DEV).astype(jnp.int32), EDGES_DEV, 1)])
        negative_pair = jnp.stack([lax.dynamic_slice_in_dim(negative_round, (lower * BLOCKS).astype(jnp.int32), BLOCKS, 0), lax.dynamic_slice_in_dim(negative_round, (upper * BLOCKS).astype(jnp.int32), BLOCKS, 0)])
        count_pair = jnp.stack([lax.dynamic_index_in_dim(count_round, lower, 0, keepdims=False), lax.dynamic_index_in_dim(count_round, upper, 0, keepdims=False)]).astype(jnp.int32)
        block_pair = (count_pair + BLOCK - 1) // BLOCK
        grads = jnp.zeros((2 * ENT_DEV, DIM), jnp.float32)
        grads, grad_relation = bucket_pass((grads, grad_relation), table, relations, edge_pair, negative_pair, count_pair, source_shift, target_shift, BLOCK, jnp.int32(0), (block_pair[0] + block_pair[1]).astype(jnp.int32))
        for side, which in ((lower, 0), (upper, 1)):
            offset = (side * ENT_DEV).astype(jnp.int32)
            rows = table[which * ENT_DEV:(which + 1) * ENT_DEV]
            state = lax.dynamic_slice_in_dim(entity_state, offset, ENT_DEV, 0)
            rows, state = adagrad(rows, state, grads[which * ENT_DEV:(which + 1) * ENT_DEV])
            new_entities = lax.dynamic_update_slice_in_dim(new_entities, rows, offset, 0)
            new_state = lax.dynamic_update_slice_in_dim(new_state, state, offset, 0)
        return (new_entities, new_state, grad_relation)
    start = (entities, entity_state, jnp.zeros((REL, DIM), jnp.float32))
    new_entities, new_state, grad_relation = lax.fori_loop(jnp.int32(0), jnp.int32(PARTITIONS // 2), visit_pair, start)
    return (new_entities, new_state, grad_relation)

def reference(entities, entity_state, relations, relation_state, edges, negatives, counts):
    levels = PARTITIONS.bit_length() - 1
    for round_index, bit in enumerate((levels - 1, 0)):
        entities, entity_state, grad_relation = round_pass(entities, entity_state, relations, edges[round_index], negatives[round_index], counts[round_index], 2 ** bit)
        relations, relation_state = adagrad(relations, relation_state, grad_relation)
    return (entities, entity_state, relations, relation_state)
```

```python
import jax
import jax.numpy as jnp
from jax import lax
from jax.experimental import pallas as pl
from jax.experimental.pallas import tpu as pltpu
from jax.sharding import PartitionSpec as P

RATE = 0.2
F32 = jnp.float32
BF16 = jnp.bfloat16
VMEM = pl.BlockSpec(memory_space=pltpu.VMEM)
SMEM = pl.BlockSpec(memory_space=pltpu.SMEM)
NN = (((1,), (0,)), ((), ()))
NT = (((1,), (1,)), ((), ()))
LANES = 128


def split(value):
    high = value.astype(BF16)
    return high, (value - high.astype(F32)).astype(BF16)


def dot(left, right, dims=NN):
    return lax.dot_general(left, right, dims, preferred_element_type=F32)


def dot3(left, right, dims=NN):
    return (
        dot(left[0], right[0], dims) + dot(left[0], right[1], dims) + dot(left[1], right[0], dims)
    )


def dot_exact(left, right, dims=NN):
    return dot(left[0], right, dims) + dot(left[1], right, dims)


def spots(ids, count):
    rows = lax.broadcasted_iota(jnp.int32, (count, ids.shape[1]), 0)
    return jnp.where(rows == ids, 1.0, 0.0).astype(BF16)


def call(kernel, outs, args, scratch=(), name=None):
    specs = [SMEM if kind == "smem" else VMEM for kind, _ in args]
    return pl.pallas_call(
        kernel,
        out_shape=[jax.ShapeDtypeStruct(*out) for out in outs],
        in_specs=specs,
        out_specs=[VMEM] * len(outs),
        scratch_shapes=list(scratch),
        name=name,
    )(*[value for _, value in args])


def prep_kernel(e_ref, edges_ref, et_ref, st_ref, wide):
    rows, dim = e_ref.shape
    wide[...] = jnp.zeros_like(wide)
    wide[:, :dim] = e_ref[...]
    et_ref[...] = wide[...].T[:dim]
    source = edges_ref[0, 0:1, :]
    st_ref[...] = dot_exact(split(et_ref[...]), spots(source, rows))


def rel_prep_kernel(r_ref, rt_ref, wide):
    rows, dim = r_ref.shape
    wide[...] = jnp.zeros_like(wide)
    wide[:rows, :dim] = r_ref[...]
    rt_ref[...] = wide[...].T[:dim]


def hist_kernel(neg_ref, c_ref):
    blocks, draws = neg_ref.shape
    rows = c_ref.shape[0]
    ones = jnp.ones((draws, LANES), BF16)
    for b in range(blocks):
        hits = spots(neg_ref[b : b + 1, :], rows)
        c_ref[:, b * LANES : (b + 1) * LANES] = dot(hits, ones) * (1.0 / draws)


def main_kernel(
    e_ref, et_ref, rt_ref, st_ref, edges_ref, c_ref, count_ref, gt_ref, gs_ref, h_ref, q, tmp
):
    rows, dim = e_ref.shape
    half = dim // 2
    wide = edges_ref.shape[1]
    rels = rt_ref.shape[1]
    relation = edges_ref[1:2, :]
    live = lax.broadcasted_iota(jnp.int32, (1, wide), 1) < count_ref[0]
    target = jnp.where(live, edges_ref[2:3, :], -1)
    alive = live.astype(F32)
    rel_spots = spots(relation, rels)
    tmp[...] = dot_exact(split(rt_ref[...]), rel_spots)
    s_re, s_im = st_ref[0:half, :], st_ref[half:dim, :]
    w_re, w_im = tmp[0:half, :], tmp[half:dim, :]
    q[0:half, :] = s_re * w_re - s_im * w_im
    q[half:dim, :] = s_re * w_im + s_im * w_re
    q_parts = split(q[...])
    up = jnp.zeros((dim, wide), F32)
    step = 256
    for j in range(0, rows, step):
        scores = dot3(split(e_ref[j : j + step, :]), q_parts)
        sig = 0.5 * jnp.tanh(0.5 * scores) + 0.5
        number = lax.broadcasted_iota(jnp.int32, (step, wide), 0) + j
        mark = jnp.where(number == target, 1.0, 0.0)
        weight = split(sig * (c_ref[j : j + step, :] * alive + mark) - mark)
        up = up + dot3(split(et_ref[:, j : j + step]), weight)
        gt_ref[:, j : j + step] = dot3(q_parts, weight, NT)
    q[...] = up
    u_re, u_im = q[0:half, :], q[half:dim, :]
    gs_ref[0:half, :] = u_re * w_re + u_im * w_im
    gs_ref[half:dim, :] = u_im * w_re - u_re * w_im
    tmp[0:half, :] = u_re * s_re + u_im * s_im
    tmp[half:dim, :] = u_im * s_re - u_re * s_im
    h_ref[...] = dot_exact(split(tmp[...]), rel_spots, NT)


def stepped(param, state, grad):
    new_state = state + jnp.sum(grad * grad, axis=0, keepdims=True) * (1.0 / grad.shape[0])
    return param - RATE * grad / jnp.sqrt(new_state), new_state


def update_kernel(number, et_ref, state_ref, gt_ref, gs_ref, edges_ref, e_out, state_out, et_out, *more):
    dim, rows = et_ref.shape
    source = spots(edges_ref[number, 0:1, :], rows)
    grad = gt_ref[...] + dot_exact(split(gs_ref[...]), source, NT)
    after, state = stepped(et_ref[...], state_ref[...], grad)
    state_out[...] = state
    wide = more[-1]
    wide[0:dim, :] = after
    wide[dim:, :] = jnp.zeros((wide.shape[0] - dim, rows), F32)
    e_out[...] = wide[...].T[:, :dim]
    et_out[...] = after
    if len(more) > 1:
        more[0][...] = dot_exact(split(after), spots(edges_ref[number + 1, 0:1, :], rows))


def rel_update_kernel(rt_ref, state_ref, h_ref, rt_out, state_out):
    rt_out[...], state_out[...] = stepped(rt_ref[...], state_ref[...], h_ref[...])


def rel_final_kernel(rt_ref, state_ref, h_ref, r_out, state_out, wide):
    dim = rt_ref.shape[0]
    after, state_out[...] = stepped(rt_ref[...], state_ref[...], h_ref[...])
    wide[0:dim, :] = after
    wide[dim:, :] = jnp.zeros((wide.shape[0] - dim, wide.shape[1]), F32)
    r_out[...] = wide[...].T[: r_out.shape[0], :dim]


def swapped(value, apart):
    count = lax.axis_size("dom")
    return lax.ppermute(value, "dom", [(low, low ^ (1 << apart)) for low in range(count)])


def body(entities, entity_state, relations, relation_state, edges, negatives, counts):
    rows, dim = entities.shape
    rels = relations.shape[0]
    rels_pad = -(-rels // LANES) * LANES
    rounds, _, slots = edges.shape
    levels = lax.axis_size("dom").bit_length() - 1
    dim_pad = -(-dim // LANES) * LANES
    et, st = call(
        prep_kernel,
        [((dim, rows), F32), ((dim, slots), F32)],
        [("v", entities), ("v", edges)],
        [pltpu.VMEM((rows, dim_pad), F32)],
        name="prep",
    )
    (rt,) = call(
        rel_prep_kernel,
        [((dim, rels_pad), F32)],
        [("v", relations)],
        [pltpu.VMEM((rels_pad, dim_pad), F32)],
        name="rel_prep",
    )
    state = entity_state.reshape(1, rows)
    rel_state = jnp.pad(relation_state.reshape(1, rels), ((0, 0), (0, rels_pad - rels)), constant_values=1.0)
    table = entities
    for number, bit in enumerate((levels - 1, 0)):
        their_edges = swapped(edges[number], bit)
        their_negatives = swapped(negatives[number], bit)
        their_count = swapped(counts[number], bit)
        their_rows = swapped(st, bit)
        (c,) = call(hist_kernel, [((rows, slots), F32)], [("v", their_negatives)], name=f"hist{number}")
        gt, gs, h = call(
            main_kernel,
            [((dim, rows), F32), ((dim, slots), F32), ((dim, rels_pad), F32)],
            [
                ("v", table),
                ("v", et),
                ("v", rt),
                ("v", their_rows),
                ("v", their_edges),
                ("v", c),
                ("smem", their_count),
            ],
            [pltpu.VMEM((dim, slots), F32), pltpu.VMEM((dim, slots), F32)],
            name=f"main{number}",
        )
        gs = swapped(gs, bit)
        h = lax.psum(h, "dom")
        last = number == rounds - 1
        outs = call(
            lambda *refs, number=number: update_kernel(number, *refs),
            [((rows, dim), F32), ((1, rows), F32), ((dim, rows), F32)]
            + ([] if last else [((dim, slots), F32)]),
            [("v", et), ("v", state), ("v", gt), ("v", gs), ("v", edges)],
            [pltpu.VMEM((dim_pad, rows), F32)],
            name=f"update{number}",
        )
        table, state, et = outs[:3]
        if last:
            relations, rel_state = call(
                rel_final_kernel,
                [((rels, dim), F32), ((1, rels_pad), F32)],
                [("v", rt), ("v", rel_state), ("v", h)],
                [pltpu.VMEM((dim_pad, rels_pad), F32)],
                name=f"rel_update{number}",
            )
        else:
            st = outs[3]
            rt, rel_state = call(
                rel_update_kernel,
                [((dim, rels_pad), F32), ((1, rels_pad), F32)],
                [("v", rt), ("v", rel_state), ("v", h)],
                name=f"rel_update{number}",
            )
    return table, state.reshape(rows), relations, rel_state[0, :rels]


def solution(mesh):
    return jax.shard_map(
        body,
        mesh=mesh,
        in_specs=(
            P("dom", None),
            P("dom"),
            P(),
            P(),
            P(None, None, "dom"),
            P(None, "dom", None),
            P(None, "dom"),
        ),
        out_specs=(P("dom", None), P("dom"), P(), P()),
        check_vma=False,
    )
```

```python
import jax
import jax.numpy as jnp
from jax import lax
from jax.experimental import pallas as pl
from jax.experimental.pallas import tpu as pltpu
from jax.sharding import PartitionSpec as P

RATE = 0.2
F32 = jnp.float32
BF16 = jnp.bfloat16
VMEM = pl.BlockSpec(memory_space=pltpu.VMEM)
SMEM = pl.BlockSpec(memory_space=pltpu.SMEM)
NN = (((1,), (0,)), ((), ()))
NT = (((1,), (1,)), ((), ()))
LANES = 128
SUBLANES = 8
ZS, XS, YS, CORES = 8, 4, 4, 2
PLANE = XS * YS
MESH = pl.DeviceIdType.MESH


def split(value):
    high = value.astype(BF16)
    return high, (value - high.astype(F32)).astype(BF16)


def dot(left, right, dims=NN):
    return lax.dot_general(left, right, dims, preferred_element_type=F32)


def dot3(left, right, dims=NN):
    return (
        dot(left[0], right[0], dims) + dot(left[0], right[1], dims) + dot(left[1], right[0], dims)
    )


def dot_exact(left, right, dims=NN):
    return dot(left[0], right, dims) + dot(left[1], right, dims)


def spots(ids, count):
    rows = lax.broadcasted_iota(jnp.int32, (count, ids.shape[1]), 0)
    return jnp.where(rows == ids, 1.0, 0.0).astype(BF16)


def call(kernel, outs, args, scratch=(), name=None, collective=None):
    specs = [SMEM if kind == "smem" else VMEM for kind, _ in args]
    params = None
    if collective is not None:
        params = pltpu.CompilerParams(collective_id=collective, has_side_effects=True)
    return pl.pallas_call(
        kernel,
        out_shape=[jax.ShapeDtypeStruct(*out) for out in outs],
        in_specs=specs,
        out_specs=[VMEM] * len(outs),
        scratch_shapes=list(scratch),
        compiler_params=params,
        name=name,
    )(*[value for _, value in args])


def prep_kernel(e_ref, edges_ref, et_ref, st_ref, wide):
    rows, dim = e_ref.shape
    wide[...] = jnp.zeros_like(wide)
    wide[:, :dim] = e_ref[...]
    et_ref[...] = wide[...].T[:dim]
    source = edges_ref[0, 0:1, :]
    st_ref[...] = dot_exact(split(et_ref[...]), spots(source, rows))


def rel_prep_kernel(r_ref, rt_ref, wide):
    rows, dim = r_ref.shape
    wide[...] = jnp.zeros_like(wide)
    wide[:rows, :dim] = r_ref[...]
    rt_ref[...] = wide[...].T[:dim]


def hist_kernel(neg_ref, c_ref):
    blocks, draws = neg_ref.shape
    rows = c_ref.shape[0]
    ones = jnp.ones((draws, LANES), BF16)
    for b in range(blocks):
        hits = spots(neg_ref[b : b + 1, :], rows)
        c_ref[:, b * LANES : (b + 1) * LANES] = dot(hits, ones) * (1.0 / draws)


def main_kernel(
    e_ref, et_ref, rt_ref, st_ref, edges_ref, c_ref, count_ref, gt_ref, gs_ref, h_ref, q, tmp
):
    rows, dim = e_ref.shape
    half = dim // 2
    wide = edges_ref.shape[1]
    rels = rt_ref.shape[1]
    relation = edges_ref[1:2, :]
    live = lax.broadcasted_iota(jnp.int32, (1, wide), 1) < count_ref[0]
    target = jnp.where(live, edges_ref[2:3, :], -1)
    alive = live.astype(F32)
    rel_spots = spots(relation, rels)
    tmp[...] = dot_exact(split(rt_ref[...]), rel_spots)
    s_re, s_im = st_ref[0:half, :], st_ref[half:dim, :]
    w_re, w_im = tmp[0:half, :], tmp[half:dim, :]
    q[0:half, :] = s_re * w_re - s_im * w_im
    q[half:dim, :] = s_re * w_im + s_im * w_re
    q_parts = split(q[...])
    up = jnp.zeros((dim, wide), F32)
    step = 256
    for j in range(0, rows, step):
        scores = dot3(split(e_ref[j : j + step, :]), q_parts)
        sig = 0.5 * jnp.tanh(0.5 * scores) + 0.5
        number = lax.broadcasted_iota(jnp.int32, (step, wide), 0) + j
        mark = jnp.where(number == target, 1.0, 0.0)
        weight = split(sig * (c_ref[j : j + step, :] * alive + mark) - mark)
        up = up + dot3(split(et_ref[:, j : j + step]), weight)
        gt_ref[:, j : j + step] = dot3(q_parts, weight, NT)
    q[...] = up
    u_re, u_im = q[0:half, :], q[half:dim, :]
    gs_ref[0:half, :] = u_re * w_re + u_im * w_im
    gs_ref[half:dim, :] = u_im * w_re - u_re * w_im
    tmp[0:half, :] = u_re * s_re + u_im * s_im
    tmp[half:dim, :] = u_im * s_re - u_re * s_im
    total = dot_exact(split(tmp[...]), rel_spots, NT)
    places, tiles = tile_places(h_ref.shape, total.shape)
    for place, (row, lane) in zip(places, tiles):
        h_ref[place] = total[row : row + SUBLANES, lane : lane + LANES]
    for place in places[len(tiles) :]:
        h_ref[place] = jnp.zeros((SUBLANES, LANES), F32)


def tile_places(shape, flat):
    places = [(c, k, t) for c in range(shape[0]) for k in range(shape[1]) for t in range(shape[2])]
    tiles = [(r, l) for r in range(0, flat[0], SUBLANES) for l in range(0, flat[1], LANES)]
    return places, tiles


def join_tiles(h_ref, whole):
    places, tiles = tile_places(h_ref.shape, whole.shape)
    for place, (row, lane) in zip(places, tiles):
        whole[row : row + SUBLANES, lane : lane + LANES] = h_ref[place]


def places_of():
    me = lax.axis_index("dom")
    return me % CORES, me // CORES % YS, me // (CORES * YS) % XS, me // (CORES * YS * XS)


def device(z, x, y, c):
    return (((z * XS + x) * YS + y) * CORES + c,)


def remote(src, dst, sems, k, to):
    return pltpu.make_async_remote_copy(
        src_ref=src,
        dst_ref=dst,
        send_sem=sems[0].at[k],
        recv_sem=sems[1].at[k],
        device_id=to,
        device_id_type=MESH,
    )


def meet(peers):
    barrier = pltpu.get_barrier_semaphore()
    for peer in peers:
        pl.semaphore_signal(barrier, inc=1, device_id=peer, device_id_type=MESH)
    pl.semaphore_wait(barrier, len(peers))


def other_core():
    c, y, x, z = places_of()
    return device(z, x, y, 1 - c)


def in_plane():
    c, y, x, z = places_of()
    plane = []
    for k in range(PLANE):
        px, py = (x + k // YS) % XS, (y + k % YS) % YS
        fx, fy = (x + XS - k // YS) % XS, (y + YS - k % YS) % YS
        plane.append((device(z, px, py, c), px * YS + py, fx * YS + fy))
    return plane


def in_column():
    c, y, x, z = places_of()
    return [device((z + k) % ZS, x, y, c) for k in range(ZS)]


def core_sum_kernel(h_ref, out_ref, got, *sems):
    other = other_core()
    c = places_of()[0]
    meet([other])
    one = remote(h_ref.at[1 - c], got, sems, 0, other)
    one.start()
    one.wait()
    out_ref[...] = h_ref[c] + got[...]


def plane_sum_kernel(h_ref, out_ref, *more):
    got, sems = more[:-2], more[-2:]
    plane = in_plane()
    meet([p[0] for p in plane[1:]])
    sends = [remote(h_ref.at[plane[k][1]], got[k], sems, k, plane[k][0]) for k in range(1, PLANE)]
    for one in sends[::-1]:
        one.start()
    total = h_ref[plane[0][1]]
    for k in range(PLANE - 1, 0, -1):
        sends[k - 1].wait_recv()
        total = total + got[k][...]
    out_ref[...] = total
    for one in sends:
        one.wait_send()


def column_sum_kernel(h_ref, out_ref, level, *more):
    got, sems = more[:-2], more[-2:]
    column = in_column()
    z = places_of()[3]
    meet(column[1:])
    sends = [remote(h_ref, got[k], sems, k, column[k]) for k in range(1, ZS)]
    for k in (4, 3, 5, 2, 6, 1, 7):
        sends[k - 1].start()
    level[z] = h_ref[...]
    for k in range(1, ZS):
        sends[k - 1].wait_recv()
        level[(z + ZS - k) % ZS] = got[k][...]
    total = level[0]
    for k in range(1, ZS):
        total = total + level[k]
    out_ref[...] = total
    for one in sends:
        one.wait_send()


def plane_share_kernel(h_ref, out_ref, *more):
    got, sems = more[:-2], more[-2:]
    plane = in_plane()
    meet([p[0] for p in plane[1:]])
    sends = [remote(h_ref, got[k], sems, k, plane[k][0]) for k in range(1, PLANE)]
    for one in sends[::-1]:
        one.start()
    out_ref[plane[0][1]] = h_ref[...]
    for k in range(PLANE - 1, 0, -1):
        sends[k - 1].wait_recv()
        out_ref[plane[k][2]] = got[k][...]
    for one in sends:
        one.wait_send()


def core_share_kernel(h_ref, out_ref, got, *sems):
    other = other_core()
    c = places_of()[0]
    meet([other])
    one = remote(h_ref, got, sems, 0, other)
    one.start()
    out_ref[c] = h_ref[...]
    one.wait()
    out_ref[1 - c] = got[...]


def settings(shape, scratch, count, number):
    return dict(
        out_shape=jax.ShapeDtypeStruct(shape, F32),
        in_specs=[VMEM],
        out_specs=VMEM,
        scratch_shapes=[*scratch, pltpu.SemaphoreType.DMA((count,)), pltpu.SemaphoreType.DMA((count,))],
        compiler_params=pltpu.CompilerParams(collective_id=number, has_side_effects=True),
    )


def reduced(h, number):
    pieces = h.shape
    half, piece = pieces[1:], pieces[2:]
    base = 5 * number
    one = pltpu.VMEM(piece, F32)
    h = pl.pallas_call(core_sum_kernel, **settings(half, [pltpu.VMEM(half, F32)], 1, base))(h)
    h = pl.pallas_call(plane_sum_kernel, **settings(piece, [one] * PLANE, PLANE, base + 1))(h)
    h = pl.pallas_call(column_sum_kernel, **settings(piece, [pltpu.VMEM((ZS, *piece), F32)] + [one] * ZS, ZS, base + 2))(h)
    h = pl.pallas_call(plane_share_kernel, **settings(half, [one] * PLANE, PLANE, base + 3))(h)
    return pl.pallas_call(core_share_kernel, **settings(pieces, [pltpu.VMEM(half, F32)], 1, base + 4))(h)


def stepped(param, state, grad):
    new_state = state + jnp.sum(grad * grad, axis=0, keepdims=True) * (1.0 / grad.shape[0])
    return param - RATE * grad / jnp.sqrt(new_state), new_state


def update_kernel(number, et_ref, state_ref, gt_ref, gs_ref, edges_ref, e_out, state_out, et_out, *more):
    dim, rows = et_ref.shape
    source = spots(edges_ref[number, 0:1, :], rows)
    grad = gt_ref[...] + dot_exact(split(gs_ref[...]), source, NT)
    after, state = stepped(et_ref[...], state_ref[...], grad)
    state_out[...] = state
    wide = more[-1]
    wide[0:dim, :] = after
    wide[dim:, :] = jnp.zeros((wide.shape[0] - dim, rows), F32)
    e_out[...] = wide[...].T[:, :dim]
    et_out[...] = after
    if len(more) > 1:
        more[0][...] = dot_exact(split(after), spots(edges_ref[number + 1, 0:1, :], rows))


def rel_update_kernel(rt_ref, state_ref, h_ref, rt_out, state_out, whole):
    join_tiles(h_ref, whole)
    rt_out[...], state_out[...] = stepped(rt_ref[...], state_ref[...], whole[...])


def rel_final_kernel(rt_ref, state_ref, h_ref, r_out, state_out, wide, whole):
    dim = rt_ref.shape[0]
    join_tiles(h_ref, whole)
    after, state_out[...] = stepped(rt_ref[...], state_ref[...], whole[...])
    wide[0:dim, :] = after
    wide[dim:, :] = jnp.zeros((wide.shape[0] - dim, wide.shape[1]), F32)
    r_out[...] = wide[...].T[: r_out.shape[0], :dim]


def swapped(value, apart):
    count = lax.axis_size("dom")
    return lax.ppermute(value, "dom", [(low, low ^ (1 << apart)) for low in range(count)])


def body(entities, entity_state, relations, relation_state, edges, negatives, counts):
    rows, dim = entities.shape
    rels = relations.shape[0]
    rels_pad = -(-rels // LANES) * LANES
    rounds, _, slots = edges.shape
    levels = lax.axis_size("dom").bit_length() - 1
    dim_pad = -(-dim // LANES) * LANES
    et, st = call(
        prep_kernel,
        [((dim, rows), F32), ((dim, slots), F32)],
        [("v", entities), ("v", edges)],
        [pltpu.VMEM((rows, dim_pad), F32)],
        name="prep",
    )
    (rt,) = call(
        rel_prep_kernel,
        [((dim, rels_pad), F32)],
        [("v", relations)],
        [pltpu.VMEM((rels_pad, dim_pad), F32)],
        name="rel_prep",
    )
    tiles = dim // SUBLANES * (rels_pad // LANES)
    pieces = (CORES, PLANE, -(-tiles // (CORES * PLANE)), SUBLANES, LANES)
    state = entity_state.reshape(1, rows)
    rel_state = jnp.pad(relation_state.reshape(1, rels), ((0, 0), (0, rels_pad - rels)), constant_values=1.0)
    table = entities
    for number, bit in enumerate((levels - 1, 0)):
        their_edges = swapped(edges[number], bit)
        their_negatives = swapped(negatives[number], bit)
        their_count = swapped(counts[number], bit)
        their_rows = swapped(st, bit)
        (c,) = call(hist_kernel, [((rows, slots), F32)], [("v", their_negatives)], name=f"hist{number}")
        gt, gs, h = call(
            main_kernel,
            [((dim, rows), F32), ((dim, slots), F32), (pieces, F32)],
            [
                ("v", table),
                ("v", et),
                ("v", rt),
                ("v", their_rows),
                ("v", their_edges),
                ("v", c),
                ("smem", their_count),
            ],
            [pltpu.VMEM((dim, slots), F32), pltpu.VMEM((dim, slots), F32)],
            name=f"main{number}",
        )
        gs = swapped(gs, bit)
        h = reduced(h, number)
        last = number == rounds - 1
        outs = call(
            lambda *refs, number=number: update_kernel(number, *refs),
            [((rows, dim), F32), ((1, rows), F32), ((dim, rows), F32)]
            + ([] if last else [((dim, slots), F32)]),
            [("v", et), ("v", state), ("v", gt), ("v", gs), ("v", edges)],
            [pltpu.VMEM((dim_pad, rows), F32)],
            name=f"update{number}",
        )
        table, state, et = outs[:3]
        if last:
            relations, rel_state = call(
                rel_final_kernel,
                [((rels, dim), F32), ((1, rels_pad), F32)],
                [("v", rt), ("v", rel_state), ("v", h)],
                [pltpu.VMEM((dim_pad, rels_pad), F32), pltpu.VMEM((dim, rels_pad), F32)],
                name=f"rel_update{number}",
            )
        else:
            st = outs[3]
            rt, rel_state = call(
                rel_update_kernel,
                [((dim, rels_pad), F32), ((1, rels_pad), F32)],
                [("v", rt), ("v", rel_state), ("v", h)],
                [pltpu.VMEM((dim, rels_pad), F32)],
                name=f"rel_update{number}",
            )
    return table, state.reshape(rows), relations, rel_state[0, :rels]


def solution(mesh):
    return jax.shard_map(
        body,
        mesh=mesh,
        in_specs=(
            P("dom", None),
            P("dom"),
            P(),
            P(),
            P(None, None, "dom"),
            P(None, "dom", None),
            P(None, "dom"),
        ),
        out_specs=(P("dom", None), P("dom"), P(), P()),
        check_vma=False,
    )
```

```python
import jax
import jax.numpy as jnp
from jax import lax
from jax.experimental import pallas as pl
from jax.experimental.pallas import tpu as pltpu
from jax.sharding import PartitionSpec as P

RATE = 0.2
F32 = jnp.float32
BF16 = jnp.bfloat16
VMEM = pl.BlockSpec(memory_space=pltpu.VMEM)
SMEM = pl.BlockSpec(memory_space=pltpu.SMEM)
NN = (((1,), (0,)), ((), ()))
NT = (((1,), (1,)), ((), ()))
LANES = 128
SUBLANES = 8
ZS, XS, YS, CORES = 8, 4, 4, 2
PLANE = XS * YS
MESH = pl.DeviceIdType.MESH


def split(value):
    high = value.astype(BF16)
    return high, (value - high.astype(F32)).astype(BF16)


def dot(left, right, dims=NN):
    return lax.dot_general(left, right, dims, preferred_element_type=F32)


def dot3(left, right, dims=NN):
    return (
        dot(left[0], right[0], dims) + dot(left[0], right[1], dims) + dot(left[1], right[0], dims)
    )


def dot_exact(left, right, dims=NN):
    return dot(left[0], right, dims) + dot(left[1], right, dims)


def spots(ids, count):
    rows = lax.broadcasted_iota(jnp.int32, (count, ids.shape[1]), 0)
    return jnp.where(rows == ids, 1.0, 0.0).astype(BF16)


def call(kernel, outs, args, scratch=(), name=None, collective=None):
    specs = [SMEM if kind == "smem" else VMEM for kind, _ in args]
    params = None
    if collective is not None:
        params = pltpu.CompilerParams(collective_id=collective, has_side_effects=True)
    return pl.pallas_call(
        kernel,
        out_shape=[jax.ShapeDtypeStruct(*out) for out in outs],
        in_specs=specs,
        out_specs=[VMEM] * len(outs),
        scratch_shapes=list(scratch),
        compiler_params=params,
        name=name,
    )(*[value for _, value in args])


def prep_kernel(e_ref, edges_ref, et_ref, st_ref, wide):
    rows, dim = e_ref.shape
    wide[...] = jnp.zeros_like(wide)
    wide[:, :dim] = e_ref[...]
    et_ref[...] = wide[...].T[:dim]
    source = edges_ref[0, 0:1, :]
    st_ref[...] = dot_exact(split(et_ref[...]), spots(source, rows))


def rel_prep_kernel(r_ref, rt_ref, wide):
    rows, dim = r_ref.shape
    wide[...] = jnp.zeros_like(wide)
    wide[:rows, :dim] = r_ref[...]
    rt_ref[...] = wide[...].T[:dim]


def hist_kernel(neg_ref, c_ref):
    blocks, draws = neg_ref.shape
    rows = c_ref.shape[0]
    ones = jnp.ones((draws, LANES), BF16)
    for b in range(blocks):
        hits = spots(neg_ref[b : b + 1, :], rows)
        c_ref[:, b * LANES : (b + 1) * LANES] = dot(hits, ones) * (1.0 / draws)


def main_kernel(
    e_ref, et_ref, rt_ref, st_ref, edges_ref, c_ref, count_ref, gt_ref, gs_ref, h_ref, q, tmp
):
    rows, dim = e_ref.shape
    half = dim // 2
    wide = edges_ref.shape[1]
    rels = rt_ref.shape[1]
    relation = edges_ref[1:2, :]
    live = lax.broadcasted_iota(jnp.int32, (1, wide), 1) < count_ref[0]
    target = jnp.where(live, edges_ref[2:3, :], -1)
    alive = live.astype(F32)
    rel_spots = spots(relation, rels)
    tmp[...] = dot_exact(split(rt_ref[...]), rel_spots)
    s_re, s_im = st_ref[0:half, :], st_ref[half:dim, :]
    w_re, w_im = tmp[0:half, :], tmp[half:dim, :]
    q[0:half, :] = s_re * w_re - s_im * w_im
    q[half:dim, :] = s_re * w_im + s_im * w_re
    q_parts = split(q[...])
    up = jnp.zeros((dim, wide), F32)
    step = 256
    for j in range(0, rows, step):
        scores = dot3(split(e_ref[j : j + step, :]), q_parts)
        sig = 0.5 * jnp.tanh(0.5 * scores) + 0.5
        number = lax.broadcasted_iota(jnp.int32, (step, wide), 0) + j
        mark = jnp.where(number == target, 1.0, 0.0)
        weight = split(sig * (c_ref[j : j + step, :] * alive + mark) - mark)
        up = up + dot3(split(et_ref[:, j : j + step]), weight)
        gt_ref[:, j : j + step] = dot3(q_parts, weight, NT)
    q[...] = up
    u_re, u_im = q[0:half, :], q[half:dim, :]
    gs_ref[0:half, :] = u_re * w_re + u_im * w_im
    gs_ref[half:dim, :] = u_im * w_re - u_re * w_im
    tmp[0:half, :] = u_re * s_re + u_im * s_im
    tmp[half:dim, :] = u_im * s_re - u_re * s_im
    total = dot_exact(split(tmp[...]), rel_spots, NT)
    places, tiles = tile_places(h_ref.shape, total.shape)
    for place, (row, lane) in zip(places, tiles):
        h_ref[place] = total[row : row + SUBLANES, lane : lane + LANES]
    for place in places[len(tiles) :]:
        h_ref[place] = jnp.zeros((SUBLANES, LANES), F32)


def tile_places(shape, flat):
    places = [(c, k, t) for c in range(shape[0]) for k in range(shape[1]) for t in range(shape[2])]
    tiles = [(r, l) for r in range(0, flat[0], SUBLANES) for l in range(0, flat[1], LANES)]
    return places, tiles


def join_tiles(h_ref, whole):
    places, tiles = tile_places(h_ref.shape, whole.shape)
    for place, (row, lane) in zip(places, tiles):
        whole[row : row + SUBLANES, lane : lane + LANES] = h_ref[place]


def places_of():
    me = lax.axis_index("dom")
    return me % CORES, me // CORES % YS, me // (CORES * YS) % XS, me // (CORES * YS * XS)


def device(z, x, y, c):
    return (((z * XS + x) * YS + y) * CORES + c,)


def remote(src, dst, sems, k, to):
    return pltpu.make_async_remote_copy(
        src_ref=src,
        dst_ref=dst,
        send_sem=sems[0].at[k],
        recv_sem=sems[1].at[k],
        device_id=to,
        device_id_type=MESH,
    )


def meet(peers):
    barrier = pltpu.get_barrier_semaphore()
    for peer in peers:
        pl.semaphore_signal(barrier, inc=1, device_id=peer, device_id_type=MESH)
    pl.semaphore_wait(barrier, len(peers))


def other_core():
    c, y, x, z = places_of()
    return device(z, x, y, 1 - c)


def in_plane():
    c, y, x, z = places_of()
    plane = []
    for k in range(PLANE):
        px, py = (x + k // YS) % XS, (y + k % YS) % YS
        fx, fy = (x + XS - k // YS) % XS, (y + YS - k % YS) % YS
        plane.append((device(z, px, py, c), px * YS + py, fx * YS + fy))
    return plane


def in_column():
    c, y, x, z = places_of()
    return [device((z + k) % ZS, x, y, c) for k in range(ZS)]


def spread_sum_kernel(h_ref, out_ref, *more):
    s0, r0, s1, r1 = more[-4:]
    acc, got0, got1 = (more[i * PLANE : (i + 1) * PLANE] for i in range(3))
    other = other_core()
    plane = in_plane()
    c = places_of()[0]
    meet([other] + [p[0] for p in plane[1:]])
    order = range(PLANE - 1, -1, -1)
    first = [remote(h_ref.at[1 - c, plane[k][1]], got0[k], (s0, r0), k, other) for k in range(PLANE)]
    second = [remote(acc[k], got1[k], (s1, r1), k, plane[k][0]) for k in range(PLANE)]
    for k in order:
        first[k].start()
    for k in order:
        first[k].wait_recv()
        acc[k][...] = h_ref[c, plane[k][1]] + got0[k][...]
        if k < PLANE - 1:
            second[k + 1].start()
    total = acc[0][...]
    for k in order[:-1]:
        second[k].wait_recv()
        total = total + got1[k][...]
    out_ref[...] = total
    for one in first + second[1:]:
        one.wait_send()


def column_sum_kernel(h_ref, out_ref, level, *more):
    got, sems = more[:-2], more[-2:]
    column = in_column()
    z = places_of()[3]
    meet(column[1:])
    sends = [remote(h_ref, got[k], sems, k, column[k]) for k in range(1, ZS)]
    for k in (4, 3, 5, 2, 6, 1, 7):
        sends[k - 1].start()
    level[z] = h_ref[...]
    for k in range(1, ZS):
        sends[k - 1].wait_recv()
        level[(z + ZS - k) % ZS] = got[k][...]
    total = level[0]
    for k in range(1, ZS):
        total = total + level[k]
    out_ref[...] = total
    for one in sends:
        one.wait_send()


def spread_share_kernel(h_ref, out_ref, *more):
    s3, r3, s4, r4 = more[-4:]
    got3, got4 = (more[i * PLANE : (i + 1) * PLANE] for i in range(2))
    other = other_core()
    plane = in_plane()
    c = places_of()[0]
    meet([other] + [p[0] for p in plane[1:]])
    order = range(PLANE - 1, 0, -1)
    fourth = [remote(h_ref, got3[k], (s3, r3), k, plane[k][0]) for k in range(PLANE)]
    fifth = [remote(got3[k] if k else h_ref, got4[k], (s4, r4), k, other) for k in range(PLANE)]
    for k in order:
        fourth[k].start()
    fifth[0].start()
    out_ref[c, plane[0][1]] = h_ref[...]
    for k in order:
        fourth[k].wait_recv()
        fifth[k].start()
        out_ref[c, plane[k][2]] = got3[k][...]
    for k in [0, *order]:
        fifth[k].wait_recv()
        out_ref[1 - c, plane[k][2]] = got4[k][...]
    for one in fourth[1:] + fifth:
        one.wait_send()


def settings(shape, scratch, counts, number):
    dma = pltpu.SemaphoreType.DMA
    return dict(
        out_shape=jax.ShapeDtypeStruct(shape, F32),
        in_specs=[VMEM],
        out_specs=VMEM,
        scratch_shapes=[*scratch, *(dma((count,)) for count in counts for _ in range(2))],
        compiler_params=pltpu.CompilerParams(collective_id=number, has_side_effects=True),
    )


def reduced(h, number):
    pieces = h.shape
    piece = pieces[2:]
    base = 3 * number
    one = pltpu.VMEM(piece, F32)
    h = pl.pallas_call(spread_sum_kernel, **settings(piece, [one] * (3 * PLANE), (PLANE, PLANE), base))(h)
    h = pl.pallas_call(column_sum_kernel, **settings(piece, [pltpu.VMEM((ZS, *piece), F32)] + [one] * ZS, (ZS,), base + 1))(h)
    return pl.pallas_call(spread_share_kernel, **settings(pieces, [one] * (2 * PLANE), (PLANE, PLANE), base + 2))(h)


def stepped(param, state, grad):
    new_state = state + jnp.sum(grad * grad, axis=0, keepdims=True) * (1.0 / grad.shape[0])
    return param - RATE * grad / jnp.sqrt(new_state), new_state


def update_kernel(number, et_ref, state_ref, gt_ref, gs_ref, edges_ref, e_out, state_out, et_out, *more):
    dim, rows = et_ref.shape
    source = spots(edges_ref[number, 0:1, :], rows)
    grad = gt_ref[...] + dot_exact(split(gs_ref[...]), source, NT)
    after, state = stepped(et_ref[...], state_ref[...], grad)
    state_out[...] = state
    wide = more[-1]
    wide[0:dim, :] = after
    wide[dim:, :] = jnp.zeros((wide.shape[0] - dim, rows), F32)
    e_out[...] = wide[...].T[:, :dim]
    et_out[...] = after
    if len(more) > 1:
        more[0][...] = dot_exact(split(after), spots(edges_ref[number + 1, 0:1, :], rows))


def rel_update_kernel(rt_ref, state_ref, h_ref, rt_out, state_out, whole):
    join_tiles(h_ref, whole)
    rt_out[...], state_out[...] = stepped(rt_ref[...], state_ref[...], whole[...])


def rel_final_kernel(rt_ref, state_ref, h_ref, r_out, state_out, wide, whole):
    dim = rt_ref.shape[0]
    join_tiles(h_ref, whole)
    after, state_out[...] = stepped(rt_ref[...], state_ref[...], whole[...])
    wide[0:dim, :] = after
    wide[dim:, :] = jnp.zeros((wide.shape[0] - dim, wide.shape[1]), F32)
    r_out[...] = wide[...].T[: r_out.shape[0], :dim]


def swapped(value, apart):
    count = lax.axis_size("dom")
    return lax.ppermute(value, "dom", [(low, low ^ (1 << apart)) for low in range(count)])


def body(entities, entity_state, relations, relation_state, edges, negatives, counts):
    rows, dim = entities.shape
    rels = relations.shape[0]
    rels_pad = -(-rels // LANES) * LANES
    rounds, _, slots = edges.shape
    levels = lax.axis_size("dom").bit_length() - 1
    dim_pad = -(-dim // LANES) * LANES
    et, st = call(
        prep_kernel,
        [((dim, rows), F32), ((dim, slots), F32)],
        [("v", entities), ("v", edges)],
        [pltpu.VMEM((rows, dim_pad), F32)],
        name="prep",
    )
    (rt,) = call(
        rel_prep_kernel,
        [((dim, rels_pad), F32)],
        [("v", relations)],
        [pltpu.VMEM((rels_pad, dim_pad), F32)],
        name="rel_prep",
    )
    tiles = dim // SUBLANES * (rels_pad // LANES)
    pieces = (CORES, PLANE, -(-tiles // (CORES * PLANE)), SUBLANES, LANES)
    state = entity_state.reshape(1, rows)
    rel_state = jnp.pad(relation_state.reshape(1, rels), ((0, 0), (0, rels_pad - rels)), constant_values=1.0)
    table = entities
    for number, bit in enumerate((levels - 1, 0)):
        their_edges = swapped(edges[number], bit)
        their_negatives = swapped(negatives[number], bit)
        their_count = swapped(counts[number], bit)
        their_rows = swapped(st, bit)
        (c,) = call(hist_kernel, [((rows, slots), F32)], [("v", their_negatives)], name=f"hist{number}")
        gt, gs, h = call(
            main_kernel,
            [((dim, rows), F32), ((dim, slots), F32), (pieces, F32)],
            [
                ("v", table),
                ("v", et),
                ("v", rt),
                ("v", their_rows),
                ("v", their_edges),
                ("v", c),
                ("smem", their_count),
            ],
            [pltpu.VMEM((dim, slots), F32), pltpu.VMEM((dim, slots), F32)],
            name=f"main{number}",
        )
        gs = swapped(gs, bit)
        h = reduced(h, number)
        last = number == rounds - 1
        outs = call(
            lambda *refs, number=number: update_kernel(number, *refs),
            [((rows, dim), F32), ((1, rows), F32), ((dim, rows), F32)]
            + ([] if last else [((dim, slots), F32)]),
            [("v", et), ("v", state), ("v", gt), ("v", gs), ("v", edges)],
            [pltpu.VMEM((dim_pad, rows), F32)],
            name=f"update{number}",
        )
        table, state, et = outs[:3]
        if last:
            relations, rel_state = call(
                rel_final_kernel,
                [((rels, dim), F32), ((1, rels_pad), F32)],
                [("v", rt), ("v", rel_state), ("v", h)],
                [pltpu.VMEM((dim_pad, rels_pad), F32), pltpu.VMEM((dim, rels_pad), F32)],
                name=f"rel_update{number}",
            )
        else:
            st = outs[3]
            rt, rel_state = call(
                rel_update_kernel,
                [((dim, rels_pad), F32), ((1, rels_pad), F32)],
                [("v", rt), ("v", rel_state), ("v", h)],
                [pltpu.VMEM((dim, rels_pad), F32)],
                name=f"rel_update{number}",
            )
    return table, state.reshape(rows), relations, rel_state[0, :rels]


def solution(mesh):
    return jax.shard_map(
        body,
        mesh=mesh,
        in_specs=(
            P("dom", None),
            P("dom"),
            P(),
            P(),
            P(None, None, "dom"),
            P(None, "dom", None),
            P(None, "dom"),
        ),
        out_specs=(P("dom", None), P("dom"), P(), P()),
        check_vma=False,
    )
```

```python
import functools

import jax
import jax.numpy as jnp
from jax import lax
from jax.experimental import pallas as pl
from jax.experimental.pallas import tpu as pltpu
from jax.sharding import PartitionSpec as P

RATE = 0.2
F32 = jnp.float32
BF16 = jnp.bfloat16
VMEM = pl.BlockSpec(memory_space=pltpu.VMEM)
SMEM = pl.BlockSpec(memory_space=pltpu.SMEM)
NN = (((1,), (0,)), ((), ()))
NT = (((1,), (1,)), ((), ()))
LANES = 128
SUBLANES = 8
ZS, XS, YS, CORES = 8, 4, 4, 2
PLANE = XS * YS
MESH = pl.DeviceIdType.MESH


def split(value):
    high = value.astype(BF16)
    return high, (value - high.astype(F32)).astype(BF16)


def dot(left, right, dims=NN):
    return lax.dot_general(left, right, dims, preferred_element_type=F32)


def dot3(left, right, dims=NN):
    return (
        dot(left[0], right[0], dims) + dot(left[0], right[1], dims) + dot(left[1], right[0], dims)
    )


def dot_exact(left, right, dims=NN):
    return dot(left[0], right, dims) + dot(left[1], right, dims)


def spots(ids, count):
    rows = lax.broadcasted_iota(jnp.int32, (count, ids.shape[1]), 0)
    return jnp.where(rows == ids, 1.0, 0.0).astype(BF16)


def call(kernel, outs, args, scratch=(), name=None, collective=None):
    params = None
    if collective is not None:
        params = pltpu.CompilerParams(collective_id=collective, has_side_effects=True)
    return pl.pallas_call(
        kernel,
        out_shape=[jax.ShapeDtypeStruct(*out) for out in outs],
        in_specs=[VMEM] * len(args),
        out_specs=[VMEM] * len(outs),
        scratch_shapes=list(scratch),
        compiler_params=params,
        name=name,
    )(*args)


def pairs(*counts):
    return [pltpu.SemaphoreType.DMA((count,)) for count in counts for _ in range(2)]


def prep_kernel(e_ref, edges_ref, neg_ref, counts_ref, et_ref, st_ref, meta_ref, wide):
    rows, dim = e_ref.shape
    rounds, kinds, slots = edges_ref.shape
    blocks, draws = neg_ref.shape[1:]
    wide[...] = jnp.zeros_like(wide)
    wide[:, :dim] = e_ref[...]
    et_ref[...] = wide[...].T[:dim]
    source = edges_ref[0, 0:1, :]
    st_ref[...] = dot_exact(split(et_ref[...]), spots(source, rows))
    meta_ref[...] = jnp.full(meta_ref.shape, -1, jnp.int32)
    for r in range(rounds):
        meta_ref[r, 0:kinds, 0:slots] = edges_ref[r]
        meta_ref[r, kinds : kinds + 1, :] = jnp.broadcast_to(counts_ref[r : r + 1, :], (1, rows))
        meta_ref[r, kinds + 1 : kinds + 1 + blocks, 0:draws] = neg_ref[r]


def hist(meta_ref, c_ref, blocks, draws):
    ones = jnp.ones((meta_ref.shape[1], LANES), BF16)
    for b in range(blocks):
        hits = spots(meta_ref[4 + b : 5 + b, :], c_ref.shape[0])
        c_ref[:, b * LANES : (b + 1) * LANES] = dot(hits, ones) * (1.0 / draws)


def exchange_kernel(
    draws, st_ref, meta_ref, r_ref, rows_ref, meta0_ref, meta1_ref, rt_ref, c0_ref, c1_ref, wide, ss, rs
):
    c, y, x, z = places_of()
    far, near = device((z + ZS // 2) % ZS, x, y, c), other_core()
    meet([far, near])
    sends = [
        remote(meta_ref.at[0], meta0_ref, (ss, rs), 0, far),
        remote(meta_ref.at[1], meta1_ref, (ss, rs), 1, near),
        remote(st_ref, rows_ref, (ss, rs), 2, far),
    ]
    for one in sends:
        one.start()
    rels, dim = r_ref.shape
    blocks = c0_ref.shape[1] // LANES
    wide[...] = jnp.zeros_like(wide)
    wide[:rels, :dim] = r_ref[...]
    rt_ref[...] = wide[...].T[:dim]
    sends[1].wait_recv()
    hist(meta1_ref, c1_ref, blocks, draws)
    sends[0].wait_recv()
    hist(meta0_ref, c0_ref, blocks, draws)
    sends[2].wait_recv()
    for one in sends:
        one.wait_send()


def main_kernel(
    e_ref, et_ref, rt_ref, st_ref, meta_ref, c_ref, gt_ref, gs_ref, h_ref, q, tmp
):
    rows, dim = e_ref.shape
    half = dim // 2
    wide = st_ref.shape[1]
    rels = rt_ref.shape[1]
    relation = meta_ref[1:2, 0:wide]
    live = lax.broadcasted_iota(jnp.int32, (1, wide), 1) < meta_ref[3:4, 0:wide]
    target = jnp.where(live, meta_ref[2:3, 0:wide], -1)
    alive = live.astype(F32)
    rel_spots = spots(relation, rels)
    tmp[...] = dot_exact(split(rt_ref[...]), rel_spots)
    s_re, s_im = st_ref[0:half, :], st_ref[half:dim, :]
    w_re, w_im = tmp[0:half, :], tmp[half:dim, :]
    q[0:half, :] = s_re * w_re - s_im * w_im
    q[half:dim, :] = s_re * w_im + s_im * w_re
    q_parts = split(q[...])
    up = jnp.zeros((dim, wide), F32)
    step = 256
    for j in range(0, rows, step):
        scores = dot3(split(e_ref[j : j + step, :]), q_parts)
        sig = 0.5 * jnp.tanh(0.5 * scores) + 0.5
        number = lax.broadcasted_iota(jnp.int32, (step, wide), 0) + j
        mark = jnp.where(number == target, 1.0, 0.0)
        weight = split(sig * (c_ref[j : j + step, :] * alive + mark) - mark)
        up = up + dot3(split(et_ref[:, j : j + step]), weight)
        gt_ref[:, j : j + step] = dot3(q_parts, weight, NT)
    q[...] = up
    u_re, u_im = q[0:half, :], q[half:dim, :]
    gs_ref[0:half, :] = u_re * w_re + u_im * w_im
    gs_ref[half:dim, :] = u_im * w_re - u_re * w_im
    tmp[0:half, :] = u_re * s_re + u_im * s_im
    tmp[half:dim, :] = u_im * s_re - u_re * s_im
    total = dot_exact(split(tmp[...]), rel_spots, NT)
    places, tiles = tile_places(h_ref.shape, total.shape)
    for place, (row, lane) in zip(places, tiles):
        h_ref[place] = total[row : row + SUBLANES, lane : lane + LANES]
    for place in places[len(tiles) :]:
        h_ref[place] = jnp.zeros((SUBLANES, LANES), F32)


def second_main_kernel(
    e_ref, et_ref, rt_ref, rel_state_ref, sum_ref, st_ref, meta_ref, c_ref,
    gt_ref, gs_ref, h_ref, rt_out, rel_state_out, q, tmp, whole,
):
    join_tiles(sum_ref, whole)
    rt_out[...], rel_state_out[...] = stepped(rt_ref[...], rel_state_ref[...], whole[...])
    main_kernel(e_ref, et_ref, rt_out, st_ref, meta_ref, c_ref, gt_ref, gs_ref, h_ref, q, tmp)


def tile_places(shape, flat):
    places = [(c, k, t) for c in range(shape[0]) for k in range(shape[1]) for t in range(shape[2])]
    tiles = [(r, l) for r in range(0, flat[0], SUBLANES) for l in range(0, flat[1], LANES)]
    return places, tiles


def join_tiles(h_ref, whole):
    places, tiles = tile_places(h_ref.shape, whole.shape)
    for place, (row, lane) in zip(places, tiles):
        whole[row : row + SUBLANES, lane : lane + LANES] = h_ref[place]


def places_of():
    me = lax.axis_index("dom")
    return me % CORES, me // CORES % YS, me // (CORES * YS) % XS, me // (CORES * YS * XS)


def device(z, x, y, c):
    return (((z * XS + x) * YS + y) * CORES + c,)


def remote(src, dst, sems, k, to):
    return pltpu.make_async_remote_copy(
        src_ref=src,
        dst_ref=dst,
        send_sem=sems[0].at[k],
        recv_sem=sems[1].at[k],
        device_id=to,
        device_id_type=MESH,
    )


def meet(peers):
    barrier = pltpu.get_barrier_semaphore()
    for peer in peers:
        pl.semaphore_signal(barrier, inc=1, device_id=peer, device_id_type=MESH)
    pl.semaphore_wait(barrier, len(peers))


def other_core():
    c, y, x, z = places_of()
    return device(z, x, y, 1 - c)


def in_plane():
    c, y, x, z = places_of()
    plane = []
    for k in range(PLANE):
        px, py = (x + k // YS) % XS, (y + k % YS) % YS
        fx, fy = (x + XS - k // YS) % XS, (y + YS - k % YS) % YS
        plane.append((device(z, px, py, c), px * YS + py, fx * YS + fy))
    return plane


def in_column():
    c, y, x, z = places_of()
    return [device((z + k) % ZS, x, y, c) for k in range(ZS)]


def spread_sum(h_ref, out_ref, *more, beside=None):
    s0, r0, s1, r1 = more[-4:]
    acc, got0, got1 = (more[i * PLANE : (i + 1) * PLANE] for i in range(3))
    other = other_core()
    plane = in_plane()
    c = places_of()[0]
    meet([other] + [p[0] for p in plane[1:]])
    order = range(PLANE - 1, -1, -1)
    first = [remote(h_ref.at[1 - c, plane[k][1]], got0[k], (s0, r0), k, other) for k in range(PLANE)]
    second = [None] + [remote(acc[k], got1[k], (s1, r1), k, plane[k][0]) for k in range(1, PLANE)]
    for k in order:
        first[k].start()
    if beside is not None:
        beside.start()
    for k in order:
        first[k].wait_recv()
        acc[k][...] = h_ref[c, plane[k][1]] + got0[k][...]
        if k < PLANE - 1:
            second[k + 1].start()
    total = acc[0][...]
    for k in order[:-1]:
        second[k].wait_recv()
        total = total + got1[k][...]
    out_ref[...] = total
    for one in first + second[1:]:
        one.wait_send()
    if beside is not None:
        beside.wait()


def spread_sum_kernel(h_ref, out_ref, *more):
    spread_sum(h_ref, out_ref, *more)


def second_spread_sum_kernel(h_ref, gs_ref, out_ref, gs_out, sx, rx, *more):
    spread_sum(h_ref, out_ref, *more, beside=remote(gs_ref, gs_out, (sx, rx), 0, other_core()))


def column_sum_kernel(h_ref, out_ref, level, *more, beside=None):
    got, sems = more[:-2], more[-2:]
    column = in_column()
    z = places_of()[3]
    meet(column[1:])
    sends = [remote(h_ref, got[k], sems, k, column[k]) for k in range(1, ZS)]
    for k in (4, 3, 5, 2, 6, 1, 7):
        sends[k - 1].start()
    level[z] = h_ref[...]
    if beside is not None:
        beside()
    for k in range(1, ZS):
        sends[k - 1].wait_recv()
        level[(z + ZS - k) % ZS] = got[k][...]
    total = level[0]
    for k in range(1, ZS):
        total = total + level[k]
    out_ref[...] = total
    for one in sends:
        one.wait_send()


def last_column_sum_kernel(
    h_ref, et_ref, state_ref, gt_ref, gs_ref, meta_ref, out_ref, e_out, state_out, wide, *more
):
    def beside():
        after = entity_step(1, et_ref, state_ref, gt_ref, gs_ref, meta_ref, state_out)
        e_out[...] = turned(after, wide)

    column_sum_kernel(h_ref, out_ref, *more, beside=beside)


def spread_share(h_ref, out_ref, *more, beside=None):
    s3, r3, s4, r4 = more[-4:]
    got3, got4 = (more[i * PLANE : (i + 1) * PLANE] for i in range(2))
    other = other_core()
    plane = in_plane()
    c = places_of()[0]
    meet([other] + [p[0] for p in plane[1:]])
    order = range(PLANE - 1, 0, -1)
    fourth = [None] + [remote(h_ref, got3[k], (s3, r3), k, plane[k][0]) for k in range(1, PLANE)]
    fifth = [remote(got3[k] if k else h_ref, got4[k], (s4, r4), k, other) for k in range(PLANE)]
    for k in order:
        fourth[k].start()
    fifth[0].start()
    extra = beside() if beside is not None else None
    out_ref[c, plane[0][1]] = h_ref[...]
    for k in order:
        fourth[k].wait_recv()
        fifth[k].start()
        out_ref[c, plane[k][2]] = got3[k][...]
    for k in [0, *order]:
        fifth[k].wait_recv()
        out_ref[1 - c, plane[k][2]] = got4[k][...]
    for one in fourth[1:] + fifth:
        one.wait_send()
    if extra is not None:
        extra.wait()


def spread_share_kernel(
    h_ref, et_ref, state_ref, gt_ref, gs_ref, meta_ref,
    out_ref, e_out, state_out, et_out, rows_out, mine, wide, sx, rx, *more,
):
    def beside():
        after = entity_step(0, et_ref, state_ref, gt_ref, gs_ref, meta_ref, state_out)
        source = meta_ref[1, 0:1, 0 : mine.shape[1]]
        mine[...] = dot_exact(split(after), spots(source, after.shape[1]))
        send = remote(mine, rows_out, (sx, rx), 0, other_core())
        et_out[...] = after
        e_out[...] = turned(after, wide)
        send.start()
        return send

    spread_share(h_ref, out_ref, *more, beside=beside)


def last_spread_share_kernel(
    h_ref, rt_ref, rel_state_ref, r_out, rel_state_out, sums, whole, wide, *more
):
    spread_share(h_ref, sums, *more)
    join_tiles(sums, whole)
    after, rel_state_out[...] = stepped(rt_ref[...], rel_state_ref[...], whole[...])
    r_out[...] = turned(after, wide)[: r_out.shape[0]]


def turned(value, wide):
    dim = value.shape[0]
    wide[0:dim, :] = value
    wide[dim:, :] = jnp.zeros((wide.shape[0] - dim, wide.shape[1]), F32)
    return wide[...].T[:, :dim]


def entity_step(number, et_ref, state_ref, gt_ref, gs_ref, meta_ref, state_out):
    source = spots(meta_ref[number, 0:1, 0 : gs_ref.shape[1]], et_ref.shape[1])
    grad = gt_ref[...] + dot_exact(split(gs_ref[...]), source, NT)
    after, state_out[...] = stepped(et_ref[...], state_ref[...], grad)
    return after


def stepped(param, state, grad):
    new_state = state + jnp.sum(grad * grad, axis=0, keepdims=True) * (1.0 / grad.shape[0])
    return param - RATE * grad / jnp.sqrt(new_state), new_state


def swapped(value, apart):
    count = lax.axis_size("dom")
    return lax.ppermute(value, "dom", [(low, low ^ (1 << apart)) for low in range(count)])


def body(entities, entity_state, relations, relation_state, edges, negatives, counts):
    rows, dim = entities.shape
    rels = relations.shape[0]
    rels_pad = -(-rels // LANES) * LANES
    slots = edges.shape[2]
    blocks, draws = negatives.shape[1:]
    dim_pad = -(-dim // LANES) * LANES
    tiles = dim // SUBLANES * (rels_pad // LANES)
    piece = (-(-tiles // (CORES * PLANE)), SUBLANES, LANES)
    pieces = (CORES, PLANE, *piece)
    one = pltpu.VMEM(piece, F32)

    def array(*shape):
        return (shape, F32)

    def space(*shape):
        return pltpu.VMEM(shape, F32)

    meta_shape = (2, 4 + blocks, rows)
    et, st, meta = call(
        prep_kernel,
        [array(dim, rows), array(dim, slots), (meta_shape, jnp.int32)],
        [entities, edges, negatives, counts],
        [space(rows, dim_pad)],
        name="prep",
    )
    state = entity_state.reshape(1, rows)
    rel_state = jnp.pad(relation_state.reshape(1, rels), ((0, 0), (0, rels_pad - rels)), constant_values=1.0)
    their_rows, meta0, meta1, rt, c0, c1 = call(
        functools.partial(exchange_kernel, draws),
        [
            array(dim, slots),
            (meta_shape[1:], jnp.int32),
            (meta_shape[1:], jnp.int32),
            array(dim, rels_pad),
            array(rows, slots),
            array(rows, slots),
        ],
        [st, meta, relations],
        [space(rels_pad, dim_pad), *pairs(3)],
        name="exchange",
        collective=0,
    )
    gt, gs, h = call(
        main_kernel,
        [array(dim, rows), array(dim, slots), (pieces, F32)],
        [entities, et, rt, their_rows, meta0, c0],
        [space(dim, slots), space(dim, slots)],
        name="main",
    )
    levels = lax.axis_size("dom").bit_length() - 1
    gs = swapped(gs, levels - 1)
    (h,) = call(
        spread_sum_kernel, [(piece, F32)], [h], [one] * (3 * PLANE) + pairs(PLANE, PLANE), name="spread_sum", collective=1
    )
    (h,) = call(
        column_sum_kernel, [(piece, F32)], [h], [space(ZS, *piece)] + [one] * ZS + pairs(ZS), name="column_sum", collective=2
    )
    h, table, state, et, their_rows = call(
        spread_share_kernel,
        [(pieces, F32), array(rows, dim), array(1, rows), array(dim, rows), array(dim, slots)],
        [h, et, state, gt, gs, meta],
        [space(dim, slots), space(dim_pad, rows), *pairs(1)] + [one] * (2 * PLANE) + pairs(PLANE, PLANE),
        name="spread_share",
        collective=3,
    )
    gt, gs, h, rt, rel_state = call(
        second_main_kernel,
        [array(dim, rows), array(dim, slots), (pieces, F32), array(dim, rels_pad), array(1, rels_pad)],
        [table, et, rt, rel_state, h, their_rows, meta1, c1],
        [space(dim, slots), space(dim, slots), space(dim, rels_pad)],
        name="second_main",
    )
    h, gs = call(
        second_spread_sum_kernel,
        [(piece, F32), array(dim, slots)],
        [h, gs],
        pairs(1) + [one] * (3 * PLANE) + pairs(PLANE, PLANE),
        name="second_spread_sum",
        collective=4,
    )
    h, table, state = call(
        last_column_sum_kernel,
        [(piece, F32), array(rows, dim), array(1, rows)],
        [h, et, state, gt, gs, meta],
        [space(dim_pad, rows), space(ZS, *piece)] + [one] * ZS + pairs(ZS),
        name="last_column_sum",
        collective=5,
    )
    relations, rel_state = call(
        last_spread_share_kernel,
        [array(rels, dim), array(1, rels_pad)],
        [h, rt, rel_state],
        [space(*pieces), space(dim, rels_pad), space(dim_pad, rels_pad)] + [one] * (2 * PLANE) + pairs(PLANE, PLANE),
        name="last_spread_share",
        collective=6,
    )
    return table, state.reshape(rows), relations, rel_state[0, :rels]


def solution(mesh):
    return jax.shard_map(
        body,
        mesh=mesh,
        in_specs=(
            P("dom", None),
            P("dom"),
            P(),
            P(),
            P(None, None, "dom"),
            P(None, "dom", None),
            P(None, "dom"),
        ),
        out_specs=(P("dom", None), P("dom"), P(), P()),
        check_vma=False,
    )
```

```python
import functools

import jax
import jax.numpy as jnp
from jax import lax
from jax.experimental import pallas as pl
from jax.experimental.pallas import tpu as pltpu
from jax.sharding import PartitionSpec as P

RATE = 0.2
F32 = jnp.float32
BF16 = jnp.bfloat16
VMEM = pl.BlockSpec(memory_space=pltpu.VMEM)
SMEM = pl.BlockSpec(memory_space=pltpu.SMEM)
NN = (((1,), (0,)), ((), ()))
NT = (((1,), (1,)), ((), ()))
LANES = 128
SUBLANES = 8
ZS, XS, YS, CORES = 8, 4, 4, 2
PLANE = XS * YS
MESH = pl.DeviceIdType.MESH


def split(value):
    high = value.astype(BF16)
    return high, (value - high.astype(F32)).astype(BF16)


def dot(left, right, dims=NN):
    return lax.dot_general(left, right, dims, preferred_element_type=F32)


def dot3(left, right, dims=NN):
    return (
        dot(left[0], right[0], dims) + dot(left[0], right[1], dims) + dot(left[1], right[0], dims)
    )


def dot_exact(left, right, dims=NN):
    return dot(left[0], right, dims) + dot(left[1], right, dims)


def spots(ids, count):
    rows = lax.broadcasted_iota(jnp.int32, (count, ids.shape[1]), 0)
    return jnp.where(rows == ids, 1.0, 0.0).astype(BF16)


def call(kernel, outs, args, scratch=(), name=None, collective=None):
    params = None
    if collective is not None:
        params = pltpu.CompilerParams(collective_id=collective, has_side_effects=True)
    return pl.pallas_call(
        kernel,
        out_shape=[jax.ShapeDtypeStruct(*out) for out in outs],
        in_specs=[VMEM] * len(args),
        out_specs=[VMEM] * len(outs),
        scratch_shapes=list(scratch),
        compiler_params=params,
        name=name,
    )(*args)


def pairs(*counts):
    return [pltpu.SemaphoreType.DMA((count,)) for count in counts for _ in range(2)]


def prep_kernel(e_ref, edges_ref, neg_ref, counts_ref, et_ref, st_ref, meta_ref, wide):
    rows, dim = e_ref.shape
    rounds, kinds, slots = edges_ref.shape
    blocks, draws = neg_ref.shape[1:]
    wide[...] = jnp.zeros_like(wide)
    wide[:, :dim] = e_ref[...]
    et_ref[...] = wide[...].T[:dim]
    source = edges_ref[0, 0:1, :]
    st_ref[...] = dot_exact(split(et_ref[...]), spots(source, rows))
    meta_ref[...] = jnp.full(meta_ref.shape, -1, jnp.int32)
    for r in range(rounds):
        meta_ref[r, 0:kinds, 0:slots] = edges_ref[r]
        meta_ref[r, kinds : kinds + 1, :] = jnp.broadcast_to(counts_ref[r : r + 1, :], (1, rows))
        meta_ref[r, kinds + 1 : kinds + 1 + blocks, 0:draws] = neg_ref[r]


def hist(meta_ref, c_ref, blocks, draws):
    ones = jnp.ones((meta_ref.shape[1], LANES), BF16)
    for b in range(blocks):
        hits = spots(meta_ref[4 + b : 5 + b, :], c_ref.shape[0])
        c_ref[:, b * LANES : (b + 1) * LANES] = dot(hits, ones) * (1.0 / draws)


def exchange_kernel(
    draws, st_ref, meta_ref, r_ref, rows_ref, meta0_ref, meta1_ref, rt_ref, c0_ref, c1_ref, wide, ss, rs
):
    c, y, x, z = places_of()
    far, near = device((z + ZS // 2) % ZS, x, y, c), other_core()
    meet([far, near])
    sends = [
        remote(meta_ref.at[0], meta0_ref, (ss, rs), 0, far),
        remote(meta_ref.at[1], meta1_ref, (ss, rs), 1, near),
        remote(st_ref, rows_ref, (ss, rs), 2, far),
    ]
    for one in sends:
        one.start()
    rels, dim = r_ref.shape
    blocks = c0_ref.shape[1] // LANES
    wide[...] = jnp.zeros_like(wide)
    wide[:rels, :dim] = r_ref[...]
    rt_ref[...] = wide[...].T[:dim]
    sends[1].wait_recv()
    hist(meta1_ref, c1_ref, blocks, draws)
    sends[0].wait_recv()
    hist(meta0_ref, c0_ref, blocks, draws)
    sends[2].wait_recv()
    for one in sends:
        one.wait_send()


def main_kernel(
    e_ref, et_ref, rt_ref, st_ref, meta_ref, c_ref, gt_ref, gs_ref, h_ref, q, tmp
):
    rows, dim = e_ref.shape
    half = dim // 2
    wide = st_ref.shape[1]
    rels = rt_ref.shape[1]
    relation = meta_ref[1:2, 0:wide]
    live = lax.broadcasted_iota(jnp.int32, (1, wide), 1) < meta_ref[3:4, 0:wide]
    target = jnp.where(live, meta_ref[2:3, 0:wide], -1)
    alive = live.astype(F32)
    rel_spots = spots(relation, rels)
    tmp[...] = dot_exact(split(rt_ref[...]), rel_spots)
    s_re, s_im = st_ref[0:half, :], st_ref[half:dim, :]
    w_re, w_im = tmp[0:half, :], tmp[half:dim, :]
    q[0:half, :] = s_re * w_re - s_im * w_im
    q[half:dim, :] = s_re * w_im + s_im * w_re
    q_parts = split(q[...])
    up = jnp.zeros((dim, wide), F32)
    step = 256
    for j in range(0, rows, step):
        scores = dot3(split(e_ref[j : j + step, :]), q_parts)
        sig = 0.5 * jnp.tanh(0.5 * scores) + 0.5
        number = lax.broadcasted_iota(jnp.int32, (step, wide), 0) + j
        mark = jnp.where(number == target, 1.0, 0.0)
        weight = split(sig * (c_ref[j : j + step, :] * alive + mark) - mark)
        up = up + dot3(split(et_ref[:, j : j + step]), weight)
        gt_ref[:, j : j + step] = dot3(q_parts, weight, NT)
    q[...] = up
    u_re, u_im = q[0:half, :], q[half:dim, :]
    gs_ref[0:half, :] = u_re * w_re + u_im * w_im
    gs_ref[half:dim, :] = u_im * w_re - u_re * w_im
    tmp[0:half, :] = u_re * s_re + u_im * s_im
    tmp[half:dim, :] = u_im * s_re - u_re * s_im
    total = dot_exact(split(tmp[...]), rel_spots, NT)
    places, tiles = tile_places(h_ref.shape, total.shape)
    for place, (row, lane) in zip(places, tiles):
        h_ref[place] = total[row : row + SUBLANES, lane : lane + LANES]
    for place in places[len(tiles) :]:
        h_ref[place] = jnp.zeros((SUBLANES, LANES), F32)


def second_main_kernel(
    e_ref, et_ref, rt_ref, rel_state_ref, sum_ref, st_ref, meta_ref, c_ref,
    gt_ref, gs_ref, h_ref, rt_out, rel_state_out, q, tmp, whole,
):
    join_tiles(sum_ref, whole)
    rt_out[...], rel_state_out[...] = stepped(rt_ref[...], rel_state_ref[...], whole[...])
    main_kernel(e_ref, et_ref, rt_out, st_ref, meta_ref, c_ref, gt_ref, gs_ref, h_ref, q, tmp)


def tile_places(shape, flat):
    places = [(c, k, t) for c in range(shape[0]) for k in range(shape[1]) for t in range(shape[2])]
    tiles = [(r, l) for r in range(0, flat[0], SUBLANES) for l in range(0, flat[1], LANES)]
    return places, tiles


def join_tiles(h_ref, whole):
    places, tiles = tile_places(h_ref.shape, whole.shape)
    for place, (row, lane) in zip(places, tiles):
        whole[row : row + SUBLANES, lane : lane + LANES] = h_ref[place]


def places_of():
    me = lax.axis_index("dom")
    return me % CORES, me // CORES % YS, me // (CORES * YS) % XS, me // (CORES * YS * XS)


def device(z, x, y, c):
    return (((z * XS + x) * YS + y) * CORES + c,)


def remote(src, dst, sems, k, to):
    return pltpu.make_async_remote_copy(
        src_ref=src,
        dst_ref=dst,
        send_sem=sems[0].at[k],
        recv_sem=sems[1].at[k],
        device_id=to,
        device_id_type=MESH,
    )


def meet(peers):
    barrier = pltpu.get_barrier_semaphore()
    for peer in peers:
        pl.semaphore_signal(barrier, inc=1, device_id=peer, device_id_type=MESH)
    pl.semaphore_wait(barrier, len(peers))


def other_core():
    c, y, x, z = places_of()
    return device(z, x, y, 1 - c)


def in_plane():
    c, y, x, z = places_of()
    plane = []
    for k in range(PLANE):
        px, py = (x + k // YS) % XS, (y + k % YS) % YS
        fx, fy = (x + XS - k // YS) % XS, (y + YS - k % YS) % YS
        plane.append((device(z, px, py, c), px * YS + py, fx * YS + fy))
    return plane


def in_column():
    c, y, x, z = places_of()
    return [device((z + k) % ZS, x, y, c) for k in range(ZS)]


def spread_sum(h_ref, out_ref, *more, beside=None, also=()):
    s0, r0, s1, r1 = more[-4:]
    acc, got0, got1 = (more[i * PLANE : (i + 1) * PLANE] for i in range(3))
    other = other_core()
    plane = in_plane()
    c = places_of()[0]
    meet([other, *(p[0] for p in plane[1:]), *also])
    order = range(PLANE - 1, -1, -1)
    first = [remote(h_ref.at[1 - c, plane[k][1]], got0[k], (s0, r0), k, other) for k in range(PLANE)]
    second = [None] + [remote(acc[k], got1[k], (s1, r1), k, plane[k][0]) for k in range(1, PLANE)]
    for k in order:
        first[k].start()
    if beside is not None:
        beside.start()
    for k in order:
        first[k].wait_recv()
        acc[k][...] = h_ref[c, plane[k][1]] + got0[k][...]
        if k < PLANE - 1:
            second[k + 1].start()
    total = acc[0][...]
    for k in order[:-1]:
        second[k].wait_recv()
        total = total + got1[k][...]
    out_ref[...] = total
    for one in first + second[1:]:
        one.wait_send()
    if beside is not None:
        beside.wait()


def spread_sum_kernel(h_ref, out_ref, *more):
    spread_sum(h_ref, out_ref, *more)


def second_spread_sum_kernel(h_ref, gs_ref, out_ref, gs_out, sx, rx, *more):
    spread_sum(h_ref, out_ref, *more, beside=remote(gs_ref, gs_out, (sx, rx), 0, other_core()))


def column_sum_kernel(h_ref, out_ref, level, *more, beside=None):
    got, sems = more[:-2], more[-2:]
    column = in_column()
    z = places_of()[3]
    meet(column[1:])
    sends = [remote(h_ref, got[k], sems, k, column[k]) for k in range(1, ZS)]
    for k in (4, 3, 5, 2, 6, 1, 7):
        sends[k - 1].start()
    level[z] = h_ref[...]
    if beside is not None:
        beside()
    for k in range(1, ZS):
        sends[k - 1].wait_recv()
        level[(z + ZS - k) % ZS] = got[k][...]
    total = level[0]
    for k in range(1, ZS):
        total = total + level[k]
    out_ref[...] = total
    for one in sends:
        one.wait_send()


def spread_column_kernel(h_ref, out_ref, level, part, *more):
    s2, r2, *more = more
    got2, more = more[:ZS], more[ZS:]
    c, y, x, z = places_of()
    column = in_column()
    spread_sum(h_ref, part, *more, also=column[1:])
    third = [None] + [remote(part, got2[k], (s2, r2), k, column[k]) for k in range(1, ZS)]
    for k in (4, 3, 5, 2, 6, 1, 7):
        third[k].start()
    level[z] = part[...]
    for k in range(1, ZS):
        third[k].wait_recv()
        level[(z + ZS - k) % ZS] = got2[k][...]
    total = level[0]
    for k in range(1, ZS):
        total = total + level[k]
    out_ref[...] = total
    for one in third[1:]:
        one.wait_send()


def last_column_sum_kernel(
    h_ref, et_ref, state_ref, gt_ref, gs_ref, meta_ref, out_ref, e_out, state_out, wide, *more
):
    def beside():
        after = entity_step(1, et_ref, state_ref, gt_ref, gs_ref, meta_ref, state_out)
        e_out[...] = turned(after, wide)

    column_sum_kernel(h_ref, out_ref, *more, beside=beside)


def spread_share(h_ref, out_ref, *more, beside=None):
    s3, r3, s4, r4 = more[-4:]
    got3, got4 = (more[i * PLANE : (i + 1) * PLANE] for i in range(2))
    other = other_core()
    plane = in_plane()
    c = places_of()[0]
    meet([other] + [p[0] for p in plane[1:]])
    order = range(PLANE - 1, 0, -1)
    fourth = [None] + [remote(h_ref, got3[k], (s3, r3), k, plane[k][0]) for k in range(1, PLANE)]
    fifth = [remote(got3[k] if k else h_ref, got4[k], (s4, r4), k, other) for k in range(PLANE)]
    for k in order:
        fourth[k].start()
    fifth[0].start()
    extra = beside() if beside is not None else None
    out_ref[c, plane[0][1]] = h_ref[...]
    for k in order:
        fourth[k].wait_recv()
        fifth[k].start()
        out_ref[c, plane[k][2]] = got3[k][...]
    for k in [0, *order]:
        fifth[k].wait_recv()
        out_ref[1 - c, plane[k][2]] = got4[k][...]
    for one in fourth[1:] + fifth:
        one.wait_send()
    if extra is not None:
        extra.wait()


def spread_share_kernel(
    h_ref, et_ref, state_ref, gt_ref, gs_ref, meta_ref,
    out_ref, e_out, state_out, et_out, rows_out, mine, wide, sx, rx, *more,
):
    def beside():
        after = entity_step(0, et_ref, state_ref, gt_ref, gs_ref, meta_ref, state_out)
        source = meta_ref[1, 0:1, 0 : mine.shape[1]]
        mine[...] = dot_exact(split(after), spots(source, after.shape[1]))
        send = remote(mine, rows_out, (sx, rx), 0, other_core())
        et_out[...] = after
        e_out[...] = turned(after, wide)
        send.start()
        return send

    spread_share(h_ref, out_ref, *more, beside=beside)


def last_spread_share_kernel(
    h_ref, rt_ref, rel_state_ref, r_out, rel_state_out, sums, whole, wide, *more
):
    spread_share(h_ref, sums, *more)
    join_tiles(sums, whole)
    after, rel_state_out[...] = stepped(rt_ref[...], rel_state_ref[...], whole[...])
    r_out[...] = turned(after, wide)[: r_out.shape[0]]


def turned(value, wide):
    dim = value.shape[0]
    wide[0:dim, :] = value
    wide[dim:, :] = jnp.zeros((wide.shape[0] - dim, wide.shape[1]), F32)
    return wide[...].T[:, :dim]


def entity_step(number, et_ref, state_ref, gt_ref, gs_ref, meta_ref, state_out):
    source = spots(meta_ref[number, 0:1, 0 : gs_ref.shape[1]], et_ref.shape[1])
    grad = gt_ref[...] + dot_exact(split(gs_ref[...]), source, NT)
    after, state_out[...] = stepped(et_ref[...], state_ref[...], grad)
    return after


def stepped(param, state, grad):
    new_state = state + jnp.sum(grad * grad, axis=0, keepdims=True) * (1.0 / grad.shape[0])
    return param - RATE * grad / jnp.sqrt(new_state), new_state


def swapped(value, apart):
    count = lax.axis_size("dom")
    return lax.ppermute(value, "dom", [(low, low ^ (1 << apart)) for low in range(count)])


def body(entities, entity_state, relations, relation_state, edges, negatives, counts):
    rows, dim = entities.shape
    rels = relations.shape[0]
    rels_pad = -(-rels // LANES) * LANES
    slots = edges.shape[2]
    blocks, draws = negatives.shape[1:]
    dim_pad = -(-dim // LANES) * LANES
    tiles = dim // SUBLANES * (rels_pad // LANES)
    piece = (-(-tiles // (CORES * PLANE)), SUBLANES, LANES)
    pieces = (CORES, PLANE, *piece)
    one = pltpu.VMEM(piece, F32)

    def array(*shape):
        return (shape, F32)

    def space(*shape):
        return pltpu.VMEM(shape, F32)

    meta_shape = (2, 4 + blocks, rows)
    et, st, meta = call(
        prep_kernel,
        [array(dim, rows), array(dim, slots), (meta_shape, jnp.int32)],
        [entities, edges, negatives, counts],
        [space(rows, dim_pad)],
        name="prep",
    )
    state = entity_state.reshape(1, rows)
    rel_state = jnp.pad(relation_state.reshape(1, rels), ((0, 0), (0, rels_pad - rels)), constant_values=1.0)
    their_rows, meta0, meta1, rt, c0, c1 = call(
        functools.partial(exchange_kernel, draws),
        [
            array(dim, slots),
            (meta_shape[1:], jnp.int32),
            (meta_shape[1:], jnp.int32),
            array(dim, rels_pad),
            array(rows, slots),
            array(rows, slots),
        ],
        [st, meta, relations],
        [space(rels_pad, dim_pad), *pairs(3)],
        name="exchange",
        collective=0,
    )
    gt, gs, h = call(
        main_kernel,
        [array(dim, rows), array(dim, slots), (pieces, F32)],
        [entities, et, rt, their_rows, meta0, c0],
        [space(dim, slots), space(dim, slots)],
        name="main",
    )
    levels = lax.axis_size("dom").bit_length() - 1
    gs = swapped(gs, levels - 1)
    (h,) = call(
        spread_column_kernel,
        [(piece, F32)],
        [h],
        [space(ZS, *piece), one, *pairs(ZS)] + [one] * (ZS + 3 * PLANE) + pairs(PLANE, PLANE),
        name="spread_column",
        collective=1,
    )
    h, table, state, et, their_rows = call(
        spread_share_kernel,
        [(pieces, F32), array(rows, dim), array(1, rows), array(dim, rows), array(dim, slots)],
        [h, et, state, gt, gs, meta],
        [space(dim, slots), space(dim_pad, rows), *pairs(1)] + [one] * (2 * PLANE) + pairs(PLANE, PLANE),
        name="spread_share",
        collective=3,
    )
    gt, gs, h, rt, rel_state = call(
        second_main_kernel,
        [array(dim, rows), array(dim, slots), (pieces, F32), array(dim, rels_pad), array(1, rels_pad)],
        [table, et, rt, rel_state, h, their_rows, meta1, c1],
        [space(dim, slots), space(dim, slots), space(dim, rels_pad)],
        name="second_main",
    )
    h, gs = call(
        second_spread_sum_kernel,
        [(piece, F32), array(dim, slots)],
        [h, gs],
        pairs(1) + [one] * (3 * PLANE) + pairs(PLANE, PLANE),
        name="second_spread_sum",
        collective=4,
    )
    h, table, state = call(
        last_column_sum_kernel,
        [(piece, F32), array(rows, dim), array(1, rows)],
        [h, et, state, gt, gs, meta],
        [space(dim_pad, rows), space(ZS, *piece)] + [one] * ZS + pairs(ZS),
        name="last_column_sum",
        collective=5,
    )
    relations, rel_state = call(
        last_spread_share_kernel,
        [array(rels, dim), array(1, rels_pad)],
        [h, rt, rel_state],
        [space(*pieces), space(dim, rels_pad), space(dim_pad, rels_pad)] + [one] * (2 * PLANE) + pairs(PLANE, PLANE),
        name="last_spread_share",
        collective=6,
    )
    return table, state.reshape(rows), relations, rel_state[0, :rels]


def solution(mesh):
    return jax.shard_map(
        body,
        mesh=mesh,
        in_specs=(
            P("dom", None),
            P("dom"),
            P(),
            P(),
            P(None, None, "dom"),
            P(None, "dom", None),
            P(None, "dom"),
        ),
        out_specs=(P("dom", None), P("dom"), P(), P()),
        check_vma=False,
    )
```

```python
import functools

import jax
import jax.numpy as jnp
from jax import lax
from jax.experimental import pallas as pl
from jax.experimental.pallas import tpu as pltpu
from jax.sharding import PartitionSpec as P

RATE = 0.2
F32 = jnp.float32
BF16 = jnp.bfloat16
VMEM = pl.BlockSpec(memory_space=pltpu.VMEM)
SMEM = pl.BlockSpec(memory_space=pltpu.SMEM)
NN = (((1,), (0,)), ((), ()))
NT = (((1,), (1,)), ((), ()))
LANES = 128
SUBLANES = 8
ZS, XS, YS, CORES = 8, 4, 4, 2
PLANE = XS * YS
MESH = pl.DeviceIdType.MESH


def split(value):
    high = value.astype(BF16)
    return high, (value - high.astype(F32)).astype(BF16)


def dot(left, right, dims=NN):
    return lax.dot_general(left, right, dims, preferred_element_type=F32)


def dot3(left, right, dims=NN):
    return (
        dot(left[0], right[0], dims) + dot(left[0], right[1], dims) + dot(left[1], right[0], dims)
    )


def dot_exact(left, right, dims=NN):
    return dot(left[0], right, dims) + dot(left[1], right, dims)


def spots(ids, count):
    rows = lax.broadcasted_iota(jnp.int32, (count, ids.shape[1]), 0)
    return jnp.where(rows == ids, 1.0, 0.0).astype(BF16)


def call(kernel, outs, args, scratch=(), name=None, collective=None):
    params = None
    if collective is not None:
        params = pltpu.CompilerParams(collective_id=collective, has_side_effects=True)
    return pl.pallas_call(
        kernel,
        out_shape=[jax.ShapeDtypeStruct(*out) for out in outs],
        in_specs=[VMEM] * len(args),
        out_specs=[VMEM] * len(outs),
        scratch_shapes=list(scratch),
        compiler_params=params,
        name=name,
    )(*args)


def pairs(*counts):
    return [pltpu.SemaphoreType.DMA((count,)) for count in counts for _ in range(2)]


def prep_kernel(e_ref, edges_ref, neg_ref, counts_ref, et_ref, st_ref, meta_ref, wide):
    rows, dim = e_ref.shape
    rounds, kinds, slots = edges_ref.shape
    blocks, draws = neg_ref.shape[1:]
    wide[...] = jnp.zeros_like(wide)
    wide[:, :dim] = e_ref[...]
    et_ref[...] = wide[...].T[:dim]
    source = edges_ref[0, 0:1, :]
    st_ref[...] = dot_exact(split(et_ref[...]), spots(source, rows))
    meta_ref[...] = jnp.full(meta_ref.shape, -1, jnp.int32)
    for r in range(rounds):
        meta_ref[r, 0:kinds, 0:slots] = edges_ref[r]
        meta_ref[r, kinds : kinds + 1, :] = jnp.broadcast_to(counts_ref[r : r + 1, :], (1, rows))
        meta_ref[r, kinds + 1 : kinds + 1 + blocks, 0:draws] = neg_ref[r]


def hist(meta_ref, c_ref, blocks, draws):
    ones = jnp.ones((meta_ref.shape[1], LANES), BF16)
    for b in range(blocks):
        hits = spots(meta_ref[4 + b : 5 + b, :], c_ref.shape[0])
        c_ref[:, b * LANES : (b + 1) * LANES] = dot(hits, ones) * (1.0 / draws)


def exchange_kernel(
    draws, st_ref, meta_ref, r_ref, rows_ref, meta0_ref, meta1_ref, rt_ref, c0_ref, c1_ref, wide, ss, rs
):
    c, y, x, z = places_of()
    far, near = device((z + ZS // 2) % ZS, x, y, c), other_core()
    meet([far, near])
    sends = [
        remote(meta_ref.at[0], meta0_ref, (ss, rs), 0, far),
        remote(meta_ref.at[1], meta1_ref, (ss, rs), 1, near),
        remote(st_ref, rows_ref, (ss, rs), 2, far),
    ]
    for one in sends:
        one.start()
    rels, dim = r_ref.shape
    blocks = c0_ref.shape[1] // LANES
    wide[...] = jnp.zeros_like(wide)
    wide[:rels, :dim] = r_ref[...]
    rt_ref[...] = wide[...].T[:dim]
    sends[1].wait_recv()
    hist(meta1_ref, c1_ref, blocks, draws)
    sends[0].wait_recv()
    hist(meta0_ref, c0_ref, blocks, draws)
    sends[2].wait_recv()
    for one in sends:
        one.wait_send()


def main_kernel(
    e_ref, et_ref, rt_ref, st_ref, meta_ref, c_ref, gt_ref, gs_ref, h_ref, q, tmp
):
    rows, dim = e_ref.shape
    half = dim // 2
    wide = st_ref.shape[1]
    rels = rt_ref.shape[1]
    relation = meta_ref[1:2, 0:wide]
    live = lax.broadcasted_iota(jnp.int32, (1, wide), 1) < meta_ref[3:4, 0:wide]
    target = jnp.where(live, meta_ref[2:3, 0:wide], -1)
    alive = live.astype(F32)
    rel_spots = spots(relation, rels)
    tmp[...] = dot_exact(split(rt_ref[...]), rel_spots)
    s_re, s_im = st_ref[0:half, :], st_ref[half:dim, :]
    w_re, w_im = tmp[0:half, :], tmp[half:dim, :]
    q[0:half, :] = s_re * w_re - s_im * w_im
    q[half:dim, :] = s_re * w_im + s_im * w_re
    q_parts = split(q[...])
    up = jnp.zeros((dim, wide), F32)
    step = 256
    for j in range(0, rows, step):
        scores = dot3(split(e_ref[j : j + step, :]), q_parts)
        sig = 0.5 * jnp.tanh(0.5 * scores) + 0.5
        number = lax.broadcasted_iota(jnp.int32, (step, wide), 0) + j
        mark = jnp.where(number == target, 1.0, 0.0)
        weight = split(sig * (c_ref[j : j + step, :] * alive + mark) - mark)
        up = up + dot3(split(et_ref[:, j : j + step]), weight)
        gt_ref[:, j : j + step] = dot3(q_parts, weight, NT)
    q[...] = up
    u_re, u_im = q[0:half, :], q[half:dim, :]
    gs_ref[0:half, :] = u_re * w_re + u_im * w_im
    gs_ref[half:dim, :] = u_im * w_re - u_re * w_im
    tmp[0:half, :] = u_re * s_re + u_im * s_im
    tmp[half:dim, :] = u_im * s_re - u_re * s_im
    total = dot_exact(split(tmp[...]), rel_spots, NT)
    places, tiles = tile_places(h_ref.shape, total.shape)
    for place, (row, lane) in zip(places, tiles):
        h_ref[place] = total[row : row + SUBLANES, lane : lane + LANES]
    for place in places[len(tiles) :]:
        h_ref[place] = jnp.zeros((SUBLANES, LANES), F32)


def second_main_kernel(
    e_ref, et_ref, rt_ref, rel_state_ref, sum_ref, st_ref, meta_ref, c_ref,
    gt_ref, gs_ref, h_ref, rt_out, rel_state_out, q, tmp, whole,
):
    join_tiles(sum_ref, whole)
    rt_out[...], rel_state_out[...] = stepped(rt_ref[...], rel_state_ref[...], whole[...])
    main_kernel(e_ref, et_ref, rt_out, st_ref, meta_ref, c_ref, gt_ref, gs_ref, h_ref, q, tmp)


def tile_places(shape, flat):
    places = [(c, k, t) for c in range(shape[0]) for k in range(shape[1]) for t in range(shape[2])]
    tiles = [(r, l) for r in range(0, flat[0], SUBLANES) for l in range(0, flat[1], LANES)]
    return places, tiles


def join_tiles(h_ref, whole):
    places, tiles = tile_places(h_ref.shape, whole.shape)
    for place, (row, lane) in zip(places, tiles):
        whole[row : row + SUBLANES, lane : lane + LANES] = h_ref[place]


def places_of():
    me = lax.axis_index("dom")
    return me % CORES, me // CORES % YS, me // (CORES * YS) % XS, me // (CORES * YS * XS)


def device(z, x, y, c):
    return (((z * XS + x) * YS + y) * CORES + c,)


def remote(src, dst, sems, k, to):
    return pltpu.make_async_remote_copy(
        src_ref=src,
        dst_ref=dst,
        send_sem=sems[0].at[k],
        recv_sem=sems[1].at[k],
        device_id=to,
        device_id_type=MESH,
    )


def meet(peers):
    barrier = pltpu.get_barrier_semaphore()
    for peer in peers:
        pl.semaphore_signal(barrier, inc=1, device_id=peer, device_id_type=MESH)
    pl.semaphore_wait(barrier, len(peers))


def other_core():
    c, y, x, z = places_of()
    return device(z, x, y, 1 - c)


def in_plane():
    c, y, x, z = places_of()
    plane = []
    for k in range(PLANE):
        px, py = (x + k // YS) % XS, (y + k % YS) % YS
        fx, fy = (x + XS - k // YS) % XS, (y + YS - k % YS) % YS
        plane.append((device(z, px, py, c), px * YS + py, fx * YS + fy))
    return plane


def in_column():
    c, y, x, z = places_of()
    return [device((z + k) % ZS, x, y, c) for k in range(ZS)]


def spread_sum(h_ref, out_ref, *more, beside=None, also=()):
    s0, r0, s1, r1 = more[-4:]
    acc, got0, got1 = (more[i * PLANE : (i + 1) * PLANE] for i in range(3))
    other = other_core()
    plane = in_plane()
    c = places_of()[0]
    meet([other, *(p[0] for p in plane[1:]), *also])
    order = range(PLANE - 1, -1, -1)
    first = [remote(h_ref.at[1 - c, plane[k][1]], got0[k], (s0, r0), k, other) for k in range(PLANE)]
    second = [None] + [remote(acc[k], got1[k], (s1, r1), k, plane[k][0]) for k in range(1, PLANE)]
    for k in order:
        first[k].start()
    if beside is not None:
        beside.start()
    for k in order:
        first[k].wait_recv()
        acc[k][...] = h_ref[c, plane[k][1]] + got0[k][...]
        if k < PLANE - 1:
            second[k + 1].start()
    total = acc[0][...]
    for k in order[:-1]:
        second[k].wait_recv()
        total = total + got1[k][...]
    out_ref[...] = total
    for one in first + second[1:]:
        one.wait_send()
    if beside is not None:
        beside.wait()


def spread_column(h_ref, out_ref, level, part, *more, near=None, during=None):
    s2, r2, *more = more
    got2, more = more[:ZS], more[ZS:]
    c, y, x, z = places_of()
    column = in_column()
    spread_sum(h_ref, part, *more, beside=near, also=column[1:])
    third = [None] + [remote(part, got2[k], (s2, r2), k, column[k]) for k in range(1, ZS)]
    for k in (4, 3, 5, 2, 6, 1, 7):
        third[k].start()
    level[z] = part[...]
    if during is not None:
        during()
    for k in range(1, ZS):
        third[k].wait_recv()
        level[(z + ZS - k) % ZS] = got2[k][...]
    total = level[0]
    for k in range(1, ZS):
        total = total + level[k]
    out_ref[...] = total
    for one in third[1:]:
        one.wait_send()


def spread_share(h_ref, out_ref, *more, beside=None, greet=True):
    s3, r3, s4, r4 = more[-4:]
    got3, got4 = (more[i * PLANE : (i + 1) * PLANE] for i in range(2))
    other = other_core()
    plane = in_plane()
    c = places_of()[0]
    if greet:
        meet([other] + [p[0] for p in plane[1:]])
    order = range(PLANE - 1, 0, -1)
    fourth = [None] + [remote(h_ref, got3[k], (s3, r3), k, plane[k][0]) for k in range(1, PLANE)]
    fifth = [remote(got3[k] if k else h_ref, got4[k], (s4, r4), k, other) for k in range(PLANE)]
    for k in order:
        fourth[k].start()
    fifth[0].start()
    extra = beside() if beside is not None else None
    out_ref[c, plane[0][1]] = h_ref[...]
    for k in order:
        fourth[k].wait_recv()
        fifth[k].start()
        out_ref[c, plane[k][2]] = got3[k][...]
    for k in [0, *order]:
        fifth[k].wait_recv()
        out_ref[1 - c, plane[k][2]] = got4[k][...]
    for one in fourth[1:] + fifth:
        one.wait_send()
    if extra is not None:
        extra.wait()


def total_kernel(
    h_ref, et_ref, state_ref, gt_ref, gs_ref, meta_ref, rt_ref, rel_state_ref,
    e_out, state_out, r_out, rel_state_out, gs_in, both, sums, whole, wide, wide_rels, sx, rx, *more,
):
    def during():
        after = entity_step(1, et_ref, state_ref, gt_ref, gs_in, meta_ref, state_out)
        e_out[...] = turned(after, wide)

    near = remote(gs_ref, gs_in, (sx, rx), 0, other_core())
    more, share = more[: -2 * PLANE - 4], more[-2 * PLANE - 4 :]
    spread_column(h_ref, both, *more, near=near, during=during)
    spread_share(both, sums, *share, greet=False)
    join_tiles(sums, whole)
    after, rel_state_out[...] = stepped(rt_ref[...], rel_state_ref[...], whole[...])
    r_out[...] = turned(after, wide_rels)[: r_out.shape[0]]


def spread_column_kernel(h_ref, out_ref, *more):
    spread_column(h_ref, out_ref, *more)


def spread_share_kernel(
    h_ref, et_ref, state_ref, gt_ref, gs_ref, meta_ref,
    out_ref, e_out, state_out, et_out, rows_out, mine, wide, sx, rx, *more,
):
    def beside():
        after = entity_step(0, et_ref, state_ref, gt_ref, gs_ref, meta_ref, state_out)
        source = meta_ref[1, 0:1, 0 : mine.shape[1]]
        mine[...] = dot_exact(split(after), spots(source, after.shape[1]))
        send = remote(mine, rows_out, (sx, rx), 0, other_core())
        et_out[...] = after
        e_out[...] = turned(after, wide)
        send.start()
        return send

    spread_share(h_ref, out_ref, *more, beside=beside)


def turned(value, wide):
    dim = value.shape[0]
    wide[0:dim, :] = value
    wide[dim:, :] = jnp.zeros((wide.shape[0] - dim, wide.shape[1]), F32)
    return wide[...].T[:, :dim]


def entity_step(number, et_ref, state_ref, gt_ref, gs_ref, meta_ref, state_out):
    source = spots(meta_ref[number, 0:1, 0 : gs_ref.shape[1]], et_ref.shape[1])
    grad = gt_ref[...] + dot_exact(split(gs_ref[...]), source, NT)
    after, state_out[...] = stepped(et_ref[...], state_ref[...], grad)
    return after


def stepped(param, state, grad):
    new_state = state + jnp.sum(grad * grad, axis=0, keepdims=True) * (1.0 / grad.shape[0])
    return param - RATE * grad / jnp.sqrt(new_state), new_state


def swapped(value, apart):
    count = lax.axis_size("dom")
    return lax.ppermute(value, "dom", [(low, low ^ (1 << apart)) for low in range(count)])


def body(entities, entity_state, relations, relation_state, edges, negatives, counts):
    rows, dim = entities.shape
    rels = relations.shape[0]
    rels_pad = -(-rels // LANES) * LANES
    slots = edges.shape[2]
    blocks, draws = negatives.shape[1:]
    dim_pad = -(-dim // LANES) * LANES
    tiles = dim // SUBLANES * (rels_pad // LANES)
    piece = (-(-tiles // (CORES * PLANE)), SUBLANES, LANES)
    pieces = (CORES, PLANE, *piece)
    one = pltpu.VMEM(piece, F32)

    def array(*shape):
        return (shape, F32)

    def space(*shape):
        return pltpu.VMEM(shape, F32)

    meta_shape = (2, 4 + blocks, rows)
    et, st, meta = call(
        prep_kernel,
        [array(dim, rows), array(dim, slots), (meta_shape, jnp.int32)],
        [entities, edges, negatives, counts],
        [space(rows, dim_pad)],
        name="prep",
    )
    state = entity_state.reshape(1, rows)
    rel_state = jnp.pad(relation_state.reshape(1, rels), ((0, 0), (0, rels_pad - rels)), constant_values=1.0)
    their_rows, meta0, meta1, rt, c0, c1 = call(
        functools.partial(exchange_kernel, draws),
        [
            array(dim, slots),
            (meta_shape[1:], jnp.int32),
            (meta_shape[1:], jnp.int32),
            array(dim, rels_pad),
            array(rows, slots),
            array(rows, slots),
        ],
        [st, meta, relations],
        [space(rels_pad, dim_pad), *pairs(3)],
        name="exchange",
        collective=0,
    )
    gt, gs, h = call(
        main_kernel,
        [array(dim, rows), array(dim, slots), (pieces, F32)],
        [entities, et, rt, their_rows, meta0, c0],
        [space(dim, slots), space(dim, slots)],
        name="main",
    )
    levels = lax.axis_size("dom").bit_length() - 1
    gs = swapped(gs, levels - 1)
    (h,) = call(
        spread_column_kernel,
        [(piece, F32)],
        [h],
        [space(ZS, *piece), one, *pairs(ZS)] + [one] * (ZS + 3 * PLANE) + pairs(PLANE, PLANE),
        name="spread_column",
        collective=1,
    )
    h, table, state, et, their_rows = call(
        spread_share_kernel,
        [(pieces, F32), array(rows, dim), array(1, rows), array(dim, rows), array(dim, slots)],
        [h, et, state, gt, gs, meta],
        [space(dim, slots), space(dim_pad, rows), *pairs(1)] + [one] * (2 * PLANE) + pairs(PLANE, PLANE),
        name="spread_share",
        collective=2,
    )
    gt, gs, h, rt, rel_state = call(
        second_main_kernel,
        [array(dim, rows), array(dim, slots), (pieces, F32), array(dim, rels_pad), array(1, rels_pad)],
        [table, et, rt, rel_state, h, their_rows, meta1, c1],
        [space(dim, slots), space(dim, slots), space(dim, rels_pad)],
        name="second_main",
    )
    table, state, relations, rel_state = call(
        total_kernel,
        [array(rows, dim), array(1, rows), array(rels, dim), array(1, rels_pad)],
        [h, et, state, gt, gs, meta, rt, rel_state],
        [space(dim, slots), one, space(*pieces), space(dim, rels_pad), space(dim_pad, rows)]
        + [space(dim_pad, rels_pad), *pairs(1), space(ZS, *piece), one, *pairs(ZS)]
        + [one] * (ZS + 3 * PLANE)
        + pairs(PLANE, PLANE)
        + [one] * (2 * PLANE)
        + pairs(PLANE, PLANE),
        name="total",
        collective=3,
    )
    return table, state.reshape(rows), relations, rel_state[0, :rels]


def solution(mesh):
    return jax.shard_map(
        body,
        mesh=mesh,
        in_specs=(
            P("dom", None),
            P("dom"),
            P(),
            P(),
            P(None, None, "dom"),
            P(None, "dom", None),
            P(None, "dom"),
        ),
        out_specs=(P("dom", None), P("dom"), P(), P()),
        check_vma=False,
    )
```

```python
import functools

import jax
import jax.numpy as jnp
from jax import lax
from jax.experimental import pallas as pl
from jax.experimental.pallas import tpu as pltpu
from jax.sharding import PartitionSpec as P

RATE = 0.2
F32 = jnp.float32
BF16 = jnp.bfloat16
VMEM = pl.BlockSpec(memory_space=pltpu.VMEM)
SMEM = pl.BlockSpec(memory_space=pltpu.SMEM)
NN = (((1,), (0,)), ((), ()))
NT = (((1,), (1,)), ((), ()))
LANES = 128
SUBLANES = 8
ZS, XS, YS, CORES = 8, 4, 4, 2
PLANE = XS * YS
MESH = pl.DeviceIdType.MESH


def split(value):
    high = value.astype(BF16)
    return high, (value - high.astype(F32)).astype(BF16)


def dot(left, right, dims=NN):
    return lax.dot_general(left, right, dims, preferred_element_type=F32)


def dot3(left, right, dims=NN):
    return (
        dot(left[0], right[0], dims) + dot(left[0], right[1], dims) + dot(left[1], right[0], dims)
    )


def dot_exact(left, right, dims=NN):
    return dot(left[0], right, dims) + dot(left[1], right, dims)


def spots(ids, count):
    rows = lax.broadcasted_iota(jnp.int32, (count, ids.shape[1]), 0)
    return jnp.where(rows == ids, 1.0, 0.0).astype(BF16)


def call(kernel, outs, args, scratch=(), name=None, collective=None):
    params = None
    if collective is not None:
        params = pltpu.CompilerParams(collective_id=collective, has_side_effects=True)
    return pl.pallas_call(
        kernel,
        out_shape=[jax.ShapeDtypeStruct(*out) for out in outs],
        in_specs=[VMEM] * len(args),
        out_specs=[VMEM] * len(outs),
        scratch_shapes=list(scratch),
        compiler_params=params,
        name=name,
    )(*args)


def pairs(*counts):
    return [pltpu.SemaphoreType.DMA((count,)) for count in counts for _ in range(2)]


def hist(meta_ref, c_ref, blocks, draws):
    ones = jnp.ones((meta_ref.shape[1], LANES), BF16)
    for b in range(blocks):
        hits = spots(meta_ref[4 + b : 5 + b, :], c_ref.shape[0])
        c_ref[:, b * LANES : (b + 1) * LANES] = dot(hits, ones) * (1.0 / draws)


def table_parts(et_ref, wide, e_parts, et_parts):
    dim = et_ref.shape[0]
    wide[0:dim, :] = et_ref[...]
    wide[dim:, :] = jnp.zeros((wide.shape[0] - dim, wide.shape[1]), F32)
    e_parts[0][...], e_parts[1][...] = split(wide[...].T)
    et_parts[0][...], et_parts[1][...] = split(et_ref[...])


def relation_rows(rt_ref, meta_ref, picks, w):
    picks[...] = spots(meta_ref[1:2, 0 : w.shape[1]], rt_ref.shape[1])
    w[...] = dot_exact(split(rt_ref[...]), picks[...])


def edge_part(part, e_parts, et_parts, st, meta_ref, c_ref, picks, w, gt_ref, gs_ref, h_sum, q, tmp):
    dim, rows = et_parts[0].shape
    half = dim // 2
    wide = st.shape[1]
    lanes = slice(part * wide, (part + 1) * wide)
    number = lax.broadcasted_iota(jnp.int32, (1, wide), 1) + part * wide
    live = number < meta_ref[3:4, lanes]
    target = jnp.where(live, meta_ref[2:3, lanes], -1)
    alive = live.astype(F32)
    s_re, s_im = st[0:half, :], st[half:dim, :]
    w_re, w_im = w[0:half, lanes], w[half:dim, lanes]
    q[0:half, :] = s_re * w_re - s_im * w_im
    q[half:dim, :] = s_re * w_im + s_im * w_re
    q_parts = split(q[...])
    up = jnp.zeros((dim, wide), F32)
    step = 256
    for j in range(0, rows, step):
        e_part = [one[j : j + step, 0:dim] for one in e_parts]
        scores = dot3(e_part, q_parts)
        sig = 0.5 * jnp.tanh(0.5 * scores) + 0.5
        row = lax.broadcasted_iota(jnp.int32, (step, wide), 0) + j
        mark = jnp.where(row == target, 1.0, 0.0)
        weight = split(sig * (c_ref[j : j + step, lanes] * alive + mark) - mark)
        up = up + dot3([one[:, j : j + step] for one in et_parts], weight)
        grad = dot3(q_parts, weight, NT)
        gt_ref[:, j : j + step] = grad if part == 0 else gt_ref[:, j : j + step] + grad
    q[...] = up
    u_re, u_im = q[0:half, :], q[half:dim, :]
    gs_ref[0:half, lanes] = u_re * w_re + u_im * w_im
    gs_ref[half:dim, lanes] = u_im * w_re - u_re * w_im
    tmp[0:half, :] = u_re * s_re + u_im * s_im
    tmp[half:dim, :] = u_im * s_re - u_re * s_im
    total = dot_exact(split(tmp[...]), picks[:, lanes], NT)
    h_sum[...] = total if part == 0 else h_sum[...] + total


def cut_tiles(h_sum, h_ref):
    places, tiles = tile_places(h_ref.shape, h_sum.shape)
    for place, (row, lane) in zip(places, tiles):
        h_ref[place] = h_sum[row : row + SUBLANES, lane : lane + LANES]
    for place in places[len(tiles) :]:
        h_ref[place] = jnp.zeros((SUBLANES, LANES), F32)


def front_kernel(
    et_ref, r_ref, edges_ref, neg_ref, counts_ref,
    gt_ref, gs_ref, h_ref, rt_ref, meta_ref, meta1_ref, c1_ref,
    meta0, c0, st, rows, wide, eh, el, eth, etl, picks, w, h_sum, q, tmp, ss, rs,
):
    dim, count = et_ref.shape
    kinds, rounds, slots = edges_ref.shape
    blocks, draws = neg_ref.shape[1:]
    parts, _, width = st.shape
    c, y, x, z = places_of()
    far, near = device((z + ZS // 2) % ZS, x, y, c), other_core()
    greet([far, near])
    eth[...], etl[...] = split(et_ref[...])
    meta_ref[...] = jnp.full(meta_ref.shape, -1, jnp.int32)
    for r in range(rounds):
        for kind in range(kinds):
            meta_ref[r, kind : kind + 1, 0:slots] = edges_ref[kind, r : r + 1, :]
        meta_ref[r, kinds : kinds + 1, :] = jnp.broadcast_to(counts_ref[0:1, r : r + 1], (1, count))
        meta_ref[r, kinds + 1 : kinds + 1 + blocks, 0:draws] = neg_ref[r]
    sends = [remote(st.at[p], rows.at[p], (ss, rs), p, far) for p in range(parts)]
    sends.append(remote(meta_ref.at[0], meta0, (ss, rs), parts, far))
    sends.append(remote(meta_ref.at[1], meta1_ref, (ss, rs), parts + 1, near))
    for p in range(parts):
        source = meta_ref[0, 0:1, p * width : (p + 1) * width]
        st[p] = dot_exact((eth[...], etl[...]), spots(source, count))
        if p == 0:
            await_peers([far, near])
            sends[parts].start()
            sends[parts + 1].start()
        sends[p].start()
    wide[0:dim, :] = et_ref[...]
    wide[dim:, :] = jnp.zeros((wide.shape[0] - dim, count), F32)
    eh[...], el[...] = split(wide[...].T)
    rt_ref[...] = jnp.zeros_like(rt_ref)
    rt_ref[:, 0 : r_ref.shape[1]] = r_ref[...]
    sends[parts + 1].wait_recv()
    hist(meta1_ref, c1_ref, blocks, draws)
    sends[parts].wait_recv()
    hist(meta0, c0, blocks, draws)
    relation_rows(rt_ref, meta0, picks, w)
    for p in range(parts):
        sends[p].wait_recv()
        edge_part(
            p, (eh, el), (eth, etl), rows.at[p], meta0, c0, picks, w, gt_ref, gs_ref, h_sum, q, tmp
        )
    cut_tiles(h_sum, h_ref)
    for one in sends:
        one.wait_send()


def second_main_kernel(
    et_ref, rt_ref, rel_state_ref, sum_ref, rows, meta_ref, c_ref,
    gt_ref, gs_ref, h_ref, rt_out, rel_state_out,
    wide, eh, el, eth, etl, picks, w, h_sum, q, tmp, state,
):
    rels = rel_state_ref.shape[1]
    join_tiles(sum_ref, h_sum)
    state[...] = jnp.ones_like(state)
    state[:, 0:rels] = rel_state_ref[...]
    rt_out[...], rel_state_out[...] = stepped(rt_ref[...], state[...], h_sum[...])
    table_parts(et_ref, wide, (eh, el), (eth, etl))
    relation_rows(rt_out, meta_ref, picks, w)
    for p in range(rows.shape[0]):
        edge_part(
            p, (eh, el), (eth, etl), rows.at[p], meta_ref, c_ref, picks, w, gt_ref, gs_ref, h_sum, q, tmp
        )
    cut_tiles(h_sum, h_ref)


def tile_places(shape, flat):
    places = [(c, k, t) for c in range(shape[0]) for k in range(shape[1]) for t in range(shape[2])]
    tiles = [(r, l) for r in range(0, flat[0], SUBLANES) for l in range(0, flat[1], LANES)]
    return places, tiles


def join_tiles(h_ref, whole):
    places, tiles = tile_places(h_ref.shape, whole.shape)
    for place, (row, lane) in zip(places, tiles):
        whole[row : row + SUBLANES, lane : lane + LANES] = h_ref[place]


def places_of():
    me = lax.axis_index("dom")
    return me % CORES, me // CORES % YS, me // (CORES * YS) % XS, me // (CORES * YS * XS)


def device(z, x, y, c):
    return (((z * XS + x) * YS + y) * CORES + c,)


def remote(src, dst, sems, k, to):
    return pltpu.make_async_remote_copy(
        src_ref=src,
        dst_ref=dst,
        send_sem=sems[0].at[k],
        recv_sem=sems[1].at[k],
        device_id=to,
        device_id_type=MESH,
    )


def greet(peers):
    for peer in peers:
        pl.semaphore_signal(
            pltpu.get_barrier_semaphore(), inc=1, device_id=peer, device_id_type=MESH
        )


def await_peers(peers):
    pl.semaphore_wait(pltpu.get_barrier_semaphore(), len(peers))


def meet(peers):
    greet(peers)
    await_peers(peers)


def other_core():
    c, y, x, z = places_of()
    return device(z, x, y, 1 - c)


def in_plane():
    c, y, x, z = places_of()
    plane = []
    for k in range(PLANE):
        px, py = (x + k // YS) % XS, (y + k % YS) % YS
        fx, fy = (x + XS - k // YS) % XS, (y + YS - k % YS) % YS
        plane.append((device(z, px, py, c), px * YS + py, fx * YS + fy))
    return plane


def in_column():
    c, y, x, z = places_of()
    return [device((z + k) % ZS, x, y, c) for k in range(ZS)]


def spread_sum(h_ref, out_ref, *more, beside=(), also=()):
    s0, r0, s1, r1 = more[-4:]
    acc, got0, got1 = (more[i * PLANE : (i + 1) * PLANE] for i in range(3))
    other = other_core()
    plane = in_plane()
    c = places_of()[0]
    meet([other, *(p[0] for p in plane[1:]), *also])
    order = range(PLANE - 1, -1, -1)
    first = [remote(h_ref.at[1 - c, plane[k][1]], got0[k], (s0, r0), k, other) for k in range(PLANE)]
    second = [None] + [remote(acc[k], got1[k], (s1, r1), k, plane[k][0]) for k in range(1, PLANE)]
    for k in order:
        first[k].start()
    for one in beside:
        one.start()
    for k in order:
        first[k].wait_recv()
        acc[k][...] = h_ref[c, plane[k][1]] + got0[k][...]
        if k < PLANE - 1:
            second[k + 1].start()
    total = acc[0][...]
    for k in order[:-1]:
        second[k].wait_recv()
        total = total + got1[k][...]
    out_ref[...] = total
    for one in first + second[1:]:
        one.wait_send()


def spread_column(h_ref, out_ref, level, part, *more, early=(), late=(), during=None):
    s2, r2, *more = more
    got2, more = more[:ZS], more[ZS:]
    c, y, x, z = places_of()
    column = in_column()
    spread_sum(h_ref, part, *more, beside=early, also=column[1:])
    third = [None] + [remote(part, got2[k], (s2, r2), k, column[k]) for k in range(1, ZS)]
    for k in (4, 3, 5, 2, 6, 1, 7):
        third[k].start()
    for one in late:
        one.start()
    level[z] = part[...]
    if during is not None:
        during()
    for k in range(1, ZS):
        third[k].wait_recv()
        level[(z + ZS - k) % ZS] = got2[k][...]
    total = level[0]
    for k in range(1, ZS):
        total = total + level[k]
    out_ref[...] = total
    for one in third[1:]:
        one.wait_send()


def spread_share(h_ref, out_ref, *more, beside=None):
    s3, r3, s4, r4 = more[-4:]
    got3, got4 = (more[i * PLANE : (i + 1) * PLANE] for i in range(2))
    other = other_core()
    plane = in_plane()
    c = places_of()[0]
    order = range(PLANE - 1, 0, -1)
    fourth = [None] + [remote(h_ref, got3[k], (s3, r3), k, plane[k][0]) for k in range(1, PLANE)]
    fifth = [remote(got3[k] if k else h_ref, got4[k], (s4, r4), k, other) for k in range(PLANE)]
    for k in order:
        fourth[k].start()
    fifth[0].start()
    out_ref[c, plane[0][1]] = h_ref[...]
    for k in order:
        fourth[k].wait_recv()
        fifth[k].start()
        out_ref[c, plane[k][2]] = got3[k][...]
    if beside is not None:
        beside()
    for k in [0, *order]:
        fifth[k].wait_recv()
        out_ref[1 - c, plane[k][2]] = got4[k][...]
    for one in fourth[1:] + fifth:
        one.wait_send()


def first_total_kernel(
    h_ref, et_ref, state_ref, gt_ref, gs_ref, meta_ref,
    sums_ref, et_out, state_out, rows_out,
    gs_in, mine, both, sx, rx, *more,
):
    c, y, x, z = places_of()
    far = device((z + ZS // 2) % ZS, x, y, c)
    dim = gs_ref.shape[0]
    parts, _, width = mine.shape
    cut = dim // 2 // SUBLANES * SUBLANES
    ends = [(0, cut), (cut, dim)]
    back = [remote(gs_ref.at[a:b], gs_in.at[a:b], (sx, rx), i, far) for i, (a, b) in enumerate(ends)]
    on = [remote(mine.at[p], rows_out.at[p], (sx, rx), 2 + p, other_core()) for p in range(parts)]
    more, share = more[: -2 * PLANE - 4], more[-2 * PLANE - 4 :]
    spread_column(h_ref, both, *more, early=back[:1], late=back[1:])

    def beside():
        for one in back:
            one.wait()
        after = entity_step(0, et_ref, state_ref, gt_ref, gs_in, meta_ref, state_out)
        et_out[...] = after
        pieces = split(after)
        for p in range(parts):
            source = meta_ref[1, 0:1, p * width : (p + 1) * width]
            mine[p] = dot_exact(pieces, spots(source, after.shape[1]))
            on[p].start()

    spread_share(both, sums_ref, *share, beside=beside)
    for one in on:
        one.wait()


def last_total_kernel(
    h_ref, et_ref, state_ref, gt_ref, gs_ref, meta_ref, rt_ref, rel_state_ref,
    et_out, state_out, rt_out, rel_state_out,
    gs_in, both, sums, whole, sx, rx, *more,
):
    near = remote(gs_ref, gs_in, (sx, rx), 0, other_core())

    def during():
        near.wait()
        et_out[...] = entity_step(1, et_ref, state_ref, gt_ref, gs_in, meta_ref, state_out)

    more, share = more[: -2 * PLANE - 4], more[-2 * PLANE - 4 :]
    spread_column(h_ref, both, *more, early=[near], during=during)
    spread_share(both, sums, *share)
    join_tiles(sums, whole)
    after, state = stepped(rt_ref[...], rel_state_ref[...], whole[...])
    rt_out[...] = after[:, 0 : rt_out.shape[1]]
    rel_state_out[...] = state[:, 0 : rt_out.shape[1]]


def entity_step(number, et_ref, state_ref, gt_ref, gs_ref, meta_ref, state_out):
    source = spots(meta_ref[number, 0:1, 0 : gs_ref.shape[1]], et_ref.shape[1])
    grad = gt_ref[...] + dot_exact(split(gs_ref[...]), source, NT)
    after, state_out[...] = stepped(et_ref[...], state_ref[...], grad)
    return after


def stepped(param, state, grad):
    new_state = state + jnp.sum(grad * grad, axis=0, keepdims=True) * (1.0 / grad.shape[0])
    return param - RATE * grad / jnp.sqrt(new_state), new_state


def body(entities, entity_state, relations, relation_state, edges, negatives, counts):
    rows, dim = entities.shape
    rels = relations.shape[0]
    rels_pad = -(-rels // LANES) * LANES
    slots = edges.shape[2]
    blocks, draws = negatives.shape[1:]
    dim_pad = -(-dim // LANES) * LANES
    tiles = dim // SUBLANES * (rels_pad // LANES)
    piece = (-(-tiles // (CORES * PLANE)), SUBLANES, LANES)
    pieces = (CORES, PLANE, *piece)
    halves = (2, dim, slots // 2)
    one = pltpu.VMEM(piece, F32)

    def array(*shape, kind=F32):
        return (shape, kind)

    def space(*shape, kind=F32):
        return pltpu.VMEM(shape, kind)

    def table_spaces():
        return [
            space(dim_pad, rows),
            space(rows, dim_pad, kind=BF16),
            space(rows, dim_pad, kind=BF16),
            space(dim, rows, kind=BF16),
            space(dim, rows, kind=BF16),
            space(rels_pad, slots, kind=BF16),
            space(dim, slots),
            space(dim, rels_pad),
            space(*halves[1:]),
            space(*halves[1:]),
        ]

    def total_spaces():
        return (
            [space(ZS, *piece), one, *pairs(ZS)]
            + [one] * (ZS + 3 * PLANE)
            + pairs(PLANE, PLANE)
            + [one] * (2 * PLANE)
            + pairs(PLANE, PLANE)
        )

    meta_shape = (2, 4 + blocks, rows)
    grads = [array(dim, rows), array(dim, slots), array(*pieces)]
    et = entities.T
    state = entity_state.reshape(1, rows)
    rel_state = relation_state.reshape(1, rels)
    gt, gs, h, rt, meta, meta1, c1 = call(
        front_kernel,
        grads
        + [
            array(dim, rels_pad),
            array(*meta_shape, kind=jnp.int32),
            array(*meta_shape[1:], kind=jnp.int32),
            array(rows, slots),
        ],
        [et, relations.T, edges.transpose(1, 0, 2), negatives, counts.T],
        [space(*meta_shape[1:], kind=jnp.int32), space(rows, slots), space(*halves), space(*halves)]
        + table_spaces()
        + pairs(4),
        name="front",
        collective=0,
    )
    h, et, state, their_rows = call(
        first_total_kernel,
        [array(*pieces), array(dim, rows), array(1, rows), array(*halves)],
        [h, et, state, gt, gs, meta],
        [space(dim, slots), space(*halves), one, *pairs(4)] + total_spaces(),
        name="first_total",
        collective=1,
    )
    gt, gs, h, rt, rel_state = call(
        second_main_kernel,
        grads + [array(dim, rels_pad), array(1, rels_pad)],
        [et, rt, rel_state, h, their_rows, meta1, c1],
        table_spaces() + [space(1, rels_pad)],
        name="second_main",
    )
    et, state, rt, rel_state = call(
        last_total_kernel,
        [array(dim, rows), array(1, rows), array(dim, rels), array(1, rels)],
        [h, et, state, gt, gs, meta, rt, rel_state],
        [space(dim, slots), one, space(*pieces), space(dim, rels_pad), *pairs(1)] + total_spaces(),
        name="last_total",
        collective=2,
    )
    return et.T, state.reshape(rows), rt.T, rel_state.reshape(rels)


def solution(mesh):
    return jax.shard_map(
        body,
        mesh=mesh,
        in_specs=(
            P("dom", None),
            P("dom"),
            P(),
            P(),
            P(None, None, "dom"),
            P(None, "dom", None),
            P(None, "dom"),
        ),
        out_specs=(P("dom", None), P("dom"), P(), P()),
        check_vma=False,
    )
```

```python
import functools

import jax
import jax.numpy as jnp
from jax import lax
from jax.experimental import pallas as pl
from jax.experimental.pallas import tpu as pltpu
from jax.sharding import PartitionSpec as P

RATE = 0.2
F32 = jnp.float32
BF16 = jnp.bfloat16
VMEM = pl.BlockSpec(memory_space=pltpu.VMEM)
SMEM = pl.BlockSpec(memory_space=pltpu.SMEM)
NN = (((1,), (0,)), ((), ()))
NT = (((1,), (1,)), ((), ()))
LANES = 128
SUBLANES = 8
ZS, XS, YS, CORES = 8, 4, 4, 2
PLANE = XS * YS
MESH = pl.DeviceIdType.MESH


def split(value):
    high = value.astype(BF16)
    return high, (value - high.astype(F32)).astype(BF16)


def dot(left, right, dims=NN):
    return lax.dot_general(left, right, dims, preferred_element_type=F32)


def dot3(left, right, dims=NN):
    return (
        dot(left[0], right[0], dims) + dot(left[0], right[1], dims) + dot(left[1], right[0], dims)
    )


def dot_exact(left, right, dims=NN):
    return dot(left[0], right, dims) + dot(left[1], right, dims)


def spots(ids, count):
    rows = lax.broadcasted_iota(jnp.int32, (count, ids.shape[1]), 0)
    return jnp.where(rows == ids, 1.0, 0.0).astype(BF16)


def call(kernel, outs, args, scratch=(), name=None, collective=None):
    params = None
    if collective is not None:
        params = pltpu.CompilerParams(collective_id=collective, has_side_effects=True)
    return pl.pallas_call(
        kernel,
        out_shape=[jax.ShapeDtypeStruct(*out) for out in outs],
        in_specs=[VMEM] * len(args),
        out_specs=[VMEM] * len(outs),
        scratch_shapes=list(scratch),
        compiler_params=params,
        name=name,
    )(*args)


def pairs(*counts):
    return [pltpu.SemaphoreType.DMA((count,)) for count in counts for _ in range(2)]


def hist(meta_ref, c_ref, blocks, draws):
    ones = jnp.ones((meta_ref.shape[1], LANES), BF16)
    for b in range(blocks):
        hits = spots(meta_ref[4 + b : 5 + b, :], c_ref.shape[0])
        c_ref[:, b * LANES : (b + 1) * LANES] = dot(hits, ones) * (1.0 / draws)


def table_parts(et_ref, wide, e_parts, et_parts):
    dim = et_ref.shape[0]
    wide[0:dim, :] = et_ref[...]
    wide[dim:, :] = jnp.zeros((wide.shape[0] - dim, wide.shape[1]), F32)
    e_parts[0][...], e_parts[1][...] = split(wide[...].T)
    et_parts[0][...], et_parts[1][...] = split(et_ref[...])


def relation_rows(rt_ref, meta_ref, picks, w):
    picks[...] = spots(meta_ref[1:2, 0 : w.shape[1]], rt_ref.shape[1])
    w[...] = dot_exact(split(rt_ref[...]), picks[...])


def edge_part(part, e_parts, et_parts, st, meta_ref, c_ref, picks, w, gt_ref, gs_ref, h_sum, q, tmp):
    dim, rows = et_parts[0].shape
    half = dim // 2
    wide = st.shape[1]
    lanes = slice(part * wide, (part + 1) * wide)
    number = lax.broadcasted_iota(jnp.int32, (1, wide), 1) + part * wide
    live = number < meta_ref[3:4, lanes]
    target = jnp.where(live, meta_ref[2:3, lanes], -1)
    alive = live.astype(F32)
    s_re, s_im = st[0:half, :], st[half:dim, :]
    w_re, w_im = w[0:half, lanes], w[half:dim, lanes]
    q[0:half, :] = s_re * w_re - s_im * w_im
    q[half:dim, :] = s_re * w_im + s_im * w_re
    q_parts = split(q[...])
    up = jnp.zeros((dim, wide), F32)
    step = 256
    for j in range(0, rows, step):
        e_part = [one[j : j + step, 0:dim] for one in e_parts]
        scores = dot3(e_part, q_parts)
        sig = 0.5 * jnp.tanh(0.5 * scores) + 0.5
        row = lax.broadcasted_iota(jnp.int32, (step, wide), 0) + j
        mark = jnp.where(row == target, 1.0, 0.0)
        weight = split(sig * (c_ref[j : j + step, lanes] * alive + mark) - mark)
        up = up + dot3([one[:, j : j + step] for one in et_parts], weight)
        grad = dot3(q_parts, weight, NT)
        gt_ref[:, j : j + step] = grad if part == 0 else gt_ref[:, j : j + step] + grad
    q[...] = up
    u_re, u_im = q[0:half, :], q[half:dim, :]
    gs_ref[0:half, lanes] = u_re * w_re + u_im * w_im
    gs_ref[half:dim, lanes] = u_im * w_re - u_re * w_im
    tmp[0:half, :] = u_re * s_re + u_im * s_im
    tmp[half:dim, :] = u_im * s_re - u_re * s_im
    total = dot_exact(split(tmp[...]), picks[:, lanes], NT)
    h_sum[...] = total if part == 0 else h_sum[...] + total


def cut_tiles(h_sum, h_ref):
    places, tiles = tile_places(h_ref.shape, h_sum.shape)
    for place, (row, lane) in zip(places, tiles):
        h_ref[place] = h_sum[row : row + SUBLANES, lane : lane + LANES]
    for place in places[len(tiles) :]:
        h_ref[place] = jnp.zeros((SUBLANES, LANES), F32)


def front(
    everyone, et_ref, r_ref, edges_ref, neg_ref, counts_ref,
    gt_ref, gs_ref, h_ref, rt_ref, meta_ref, meta1_ref, c1_ref,
    meta0, c0, st, rows, wide, eh, el, eth, etl, picks, w, h_sum, q, tmp, ss, rs,
):
    dim, count = et_ref.shape
    kinds, rounds, slots = edges_ref.shape
    blocks, draws = neg_ref.shape[1:]
    parts, _, width = st.shape
    c, y, x, z = places_of()
    far, near = device((z + ZS // 2) % ZS, x, y, c), other_core()
    greet(everyone)
    eth[...], etl[...] = split(et_ref[...])
    meta_ref[...] = jnp.full(meta_ref.shape, -1, jnp.int32)
    for r in range(rounds):
        for kind in range(kinds):
            meta_ref[r, kind : kind + 1, 0:slots] = edges_ref[kind, r : r + 1, :]
        meta_ref[r, kinds : kinds + 1, :] = jnp.broadcast_to(counts_ref[0:1, r : r + 1], (1, count))
        meta_ref[r, kinds + 1 : kinds + 1 + blocks, 0:draws] = neg_ref[r]
    sends = [remote(st.at[p], rows.at[p], (ss, rs), p, far) for p in range(parts)]
    sends.append(remote(meta_ref.at[0], meta0, (ss, rs), parts, far))
    sends.append(remote(meta_ref.at[1], meta1_ref, (ss, rs), parts + 1, near))
    for p in range(parts):
        source = meta_ref[0, 0:1, p * width : (p + 1) * width]
        st[p] = dot_exact((eth[...], etl[...]), spots(source, count))
        if p == 0:
            await_peers(everyone)
            sends[parts].start()
            sends[parts + 1].start()
        sends[p].start()
    wide[0:dim, :] = et_ref[...]
    wide[dim:, :] = jnp.zeros((wide.shape[0] - dim, count), F32)
    eh[...], el[...] = split(wide[...].T)
    rt_ref[...] = jnp.zeros_like(rt_ref)
    rt_ref[:, 0 : r_ref.shape[1]] = r_ref[...]
    sends[parts + 1].wait_recv()
    hist(meta1_ref, c1_ref, blocks, draws)
    sends[parts].wait_recv()
    hist(meta0, c0, blocks, draws)
    relation_rows(rt_ref, meta0, picks, w)
    for p in range(parts):
        sends[p].wait_recv()
        edge_part(
            p, (eh, el), (eth, etl), rows.at[p], meta0, c0, picks, w, gt_ref, gs_ref, h_sum, q, tmp
        )
    cut_tiles(h_sum, h_ref)
    for one in sends:
        one.wait_send()


def second_main(
    et_ref, rt_ref, rel_state_ref, sum_ref, rows, meta_ref, c_ref,
    gt_ref, gs_ref, h_ref, rt_out, rel_state_out,
    wide, eh, el, eth, etl, picks, w, h_sum, q, tmp,
):
    join_tiles(sum_ref, h_sum)
    rt_out[...], rel_state_out[...] = stepped(rt_ref[...], rel_state_ref[...], h_sum[...])
    table_parts(et_ref, wide, (eh, el), (eth, etl))
    relation_rows(rt_out, meta_ref, picks, w)
    for p in range(rows.shape[0]):
        edge_part(
            p, (eh, el), (eth, etl), rows.at[p], meta_ref, c_ref, picks, w, gt_ref, gs_ref, h_sum, q, tmp
        )
    cut_tiles(h_sum, h_ref)


def tile_places(shape, flat):
    places = [(c, k, t) for c in range(shape[0]) for k in range(shape[1]) for t in range(shape[2])]
    tiles = [(r, l) for r in range(0, flat[0], SUBLANES) for l in range(0, flat[1], LANES)]
    return places, tiles


def join_tiles(h_ref, whole):
    places, tiles = tile_places(h_ref.shape, whole.shape)
    for place, (row, lane) in zip(places, tiles):
        whole[row : row + SUBLANES, lane : lane + LANES] = h_ref[place]


def places_of():
    me = lax.axis_index("dom")
    return me % CORES, me // CORES % YS, me // (CORES * YS) % XS, me // (CORES * YS * XS)


def device(z, x, y, c):
    return (((z * XS + x) * YS + y) * CORES + c,)


def remote(src, dst, sems, k, to):
    return pltpu.make_async_remote_copy(
        src_ref=src,
        dst_ref=dst,
        send_sem=sems[0].at[k],
        recv_sem=sems[1].at[k],
        device_id=to,
        device_id_type=MESH,
    )


def greet(peers):
    for peer in peers:
        pl.semaphore_signal(
            pltpu.get_barrier_semaphore(), inc=1, device_id=peer, device_id_type=MESH
        )


def await_peers(peers):
    pl.semaphore_wait(pltpu.get_barrier_semaphore(), len(peers))


def other_core():
    c, y, x, z = places_of()
    return device(z, x, y, 1 - c)


def in_plane():
    c, y, x, z = places_of()
    plane = []
    for k in range(PLANE):
        px, py = (x + k // YS) % XS, (y + k % YS) % YS
        fx, fy = (x + XS - k // YS) % XS, (y + YS - k % YS) % YS
        plane.append((device(z, px, py, c), px * YS + py, fx * YS + fy))
    return plane


def in_column():
    c, y, x, z = places_of()
    return [device((z + k) % ZS, x, y, c) for k in range(ZS)]


def spread_sum(h_ref, out_ref, *more, beside=()):
    s0, r0, s1, r1 = more[-4:]
    acc, got0, got1 = (more[i * PLANE : (i + 1) * PLANE] for i in range(3))
    other = other_core()
    plane = in_plane()
    c = places_of()[0]
    order = range(PLANE - 1, -1, -1)
    first = [remote(h_ref.at[1 - c, plane[k][1]], got0[k], (s0, r0), k, other) for k in range(PLANE)]
    second = [None] + [remote(acc[k], got1[k], (s1, r1), k, plane[k][0]) for k in range(1, PLANE)]
    for k in order:
        first[k].start()
    for one in beside:
        one.start()
    for k in order:
        first[k].wait_recv()
        acc[k][...] = h_ref[c, plane[k][1]] + got0[k][...]
        if k < PLANE - 1:
            second[k + 1].start()
    total = acc[0][...]
    for k in order[:-1]:
        second[k].wait_recv()
        total = total + got1[k][...]
    out_ref[...] = total
    for one in first + second[1:]:
        one.wait_send()


def spread_column(h_ref, out_ref, level, part, *more, early=(), late=(), during=None):
    s2, r2, *more = more
    got2, more = more[:ZS], more[ZS:]
    c, y, x, z = places_of()
    column = in_column()
    spread_sum(h_ref, part, *more, beside=early)
    third = [None] + [remote(part, got2[k], (s2, r2), k, column[k]) for k in range(1, ZS)]
    for k in (4, 3, 5, 2, 6, 1, 7):
        third[k].start()
    for one in late:
        one.start()
    level[z] = part[...]
    if during is not None:
        during()
    for k in range(1, ZS):
        third[k].wait_recv()
        level[(z + ZS - k) % ZS] = got2[k][...]
    total = level[0]
    for k in range(1, ZS):
        total = total + level[k]
    out_ref[...] = total
    for one in third[1:]:
        one.wait_send()


def spread_share(h_ref, out_ref, *more, beside=None):
    s3, r3, s4, r4 = more[-4:]
    got3, got4 = (more[i * PLANE : (i + 1) * PLANE] for i in range(2))
    other = other_core()
    plane = in_plane()
    c = places_of()[0]
    order = range(PLANE - 1, 0, -1)
    fourth = [None] + [remote(h_ref, got3[k], (s3, r3), k, plane[k][0]) for k in range(1, PLANE)]
    fifth = [remote(got3[k] if k else h_ref, got4[k], (s4, r4), k, other) for k in range(PLANE)]
    for k in order:
        fourth[k].start()
    fifth[0].start()
    out_ref[c, plane[0][1]] = h_ref[...]
    for k in order:
        fourth[k].wait_recv()
        fifth[k].start()
        out_ref[c, plane[k][2]] = got3[k][...]
    if beside is not None:
        beside()
    for k in [0, *order]:
        fifth[k].wait_recv()
        out_ref[1 - c, plane[k][2]] = got4[k][...]
    for one in fourth[1:] + fifth:
        one.wait_send()


def first_total(
    h_ref, et_ref, state_ref, gt_ref, gs_ref, meta_ref,
    sums_ref, et_out, state_out, rows_out,
    gs_in, mine, both, sx, rx, *more,
):
    c, y, x, z = places_of()
    far = device((z + ZS // 2) % ZS, x, y, c)
    dim = gs_ref.shape[0]
    parts, _, width = mine.shape
    cut = dim // 2 // SUBLANES * SUBLANES
    ends = [(0, cut), (cut, dim)]
    back = [remote(gs_ref.at[a:b], gs_in.at[a:b], (sx, rx), i, far) for i, (a, b) in enumerate(ends)]
    on = [remote(mine.at[p], rows_out.at[p], (sx, rx), 2 + p, other_core()) for p in range(parts)]
    more, share = more[: -2 * PLANE - 4], more[-2 * PLANE - 4 :]
    spread_column(h_ref, both, *more, early=back[:1], late=back[1:])

    def beside():
        for one in back:
            one.wait()
        after = entity_step(0, et_ref, state_ref, gt_ref, gs_in, meta_ref, state_out)
        et_out[...] = after
        pieces = split(after)
        for p in range(parts):
            source = meta_ref[1, 0:1, p * width : (p + 1) * width]
            mine[p] = dot_exact(pieces, spots(source, after.shape[1]))
            on[p].start()

    spread_share(both, sums_ref, *share, beside=beside)
    for one in on:
        one.wait()


def last_total(
    h_ref, et_ref, state_ref, gt_ref, gs_ref, meta_ref, rt_ref, rel_state_ref,
    et_out, state_out, rt_out, rel_state_out,
    gs_in, both, sums, whole, sx, rx, *more,
):
    near = remote(gs_ref, gs_in, (sx, rx), 0, other_core())

    def during():
        near.wait()
        et_out[...] = entity_step(1, et_ref, state_ref, gt_ref, gs_in, meta_ref, state_out)

    more, share = more[: -2 * PLANE - 4], more[-2 * PLANE - 4 :]
    spread_column(h_ref, both, *more, early=[near], during=during)
    spread_share(both, sums, *share)
    join_tiles(sums, whole)
    after, state = stepped(rt_ref[...], rel_state_ref[...], whole[...])
    rt_out[...] = after[:, 0 : rt_out.shape[1]]
    rel_state_out[...] = state


def step_kernel(sizes, *refs):
    refs = list(refs)

    def take(count):
        taken, refs[:count] = refs[:count], []
        return taken

    et, state, r, rel_state, edges, neg, counts = take(7)
    et_out, state_out, rt_out, rel_state_out = take(4)
    gt, gs, h, rt, meta, meta1, c1, meta0, c0, st, rows = take(11)
    table = take(10)
    front_sems = take(2)
    sums, et1, state1, their_rows, gs_in, mine, both, sx, rx = take(9)
    first_spaces = take(sizes)
    gt1, gs1, h1, rt1, rel_state1 = take(5)
    gs_in1, both1, sums1, sx1, rx1 = take(5)
    last_spaces = take(sizes)
    everyone = [other_core()] + [one[0] for one in in_plane()[1:]] + in_column()[1:]
    front(
        everyone, et, r, edges, neg, counts, gt, gs, h, rt, meta, meta1, c1, meta0, c0, st, rows,
        *table, *front_sems,
    )
    first_total(
        h, et, state, gt, gs, meta, sums, et1, state1, their_rows, gs_in, mine, both, sx, rx,
        *first_spaces,
    )
    second_main(
        et1, rt, rel_state, sums, their_rows, meta1, c1, gt1, gs1, h1, rt1, rel_state1, *table
    )
    last_total(
        h1, et1, state1, gt1, gs1, meta, rt1, rel_state1, et_out, state_out, rt_out, rel_state_out,
        gs_in1, both1, sums1, table[7], sx1, rx1, *last_spaces,
    )


def entity_step(number, et_ref, state_ref, gt_ref, gs_ref, meta_ref, state_out):
    source = spots(meta_ref[number, 0:1, 0 : gs_ref.shape[1]], et_ref.shape[1])
    grad = gt_ref[...] + dot_exact(split(gs_ref[...]), source, NT)
    after, state_out[...] = stepped(et_ref[...], state_ref[...], grad)
    return after


def stepped(param, state, grad):
    new_state = state + jnp.sum(grad * grad, axis=0, keepdims=True) * (1.0 / grad.shape[0])
    return param - RATE * grad / jnp.sqrt(new_state), new_state


def body(entities, entity_state, relations, relation_state, edges, negatives, counts):
    rows, dim = entities.shape
    rels = relations.shape[0]
    rels_pad = -(-rels // LANES) * LANES
    slots = edges.shape[2]
    blocks, draws = negatives.shape[1:]
    dim_pad = -(-dim // LANES) * LANES
    tiles = dim // SUBLANES * (rels_pad // LANES)
    piece = (-(-tiles // (CORES * PLANE)), SUBLANES, LANES)
    pieces = (CORES, PLANE, *piece)
    halves = (2, dim, slots // 2)
    one = pltpu.VMEM(piece, F32)

    def array(*shape, kind=F32):
        return (shape, kind)

    def space(*shape, kind=F32):
        return pltpu.VMEM(shape, kind)

    def table_spaces():
        return [
            space(dim_pad, rows),
            space(rows, dim_pad, kind=BF16),
            space(rows, dim_pad, kind=BF16),
            space(dim, rows, kind=BF16),
            space(dim, rows, kind=BF16),
            space(rels_pad, slots, kind=BF16),
            space(dim, slots),
            space(dim, rels_pad),
            space(*halves[1:]),
            space(*halves[1:]),
        ]

    def total_spaces():
        return (
            [space(ZS, *piece), one, *pairs(ZS)]
            + [one] * (ZS + 3 * PLANE)
            + pairs(PLANE, PLANE)
            + [one] * (2 * PLANE)
            + pairs(PLANE, PLANE)
        )

    meta_shape = (2, 4 + blocks, rows)
    meta = space(*meta_shape, kind=jnp.int32)
    one_meta = space(*meta_shape[1:], kind=jnp.int32)
    grads = [space(dim, rows), space(dim, slots), space(*pieces)]
    scratch = [*grads, space(dim, rels_pad), meta, one_meta, space(rows, slots), one_meta]
    scratch += [space(rows, slots), space(*halves), space(*halves), *table_spaces(), *pairs(4)]
    scratch += [space(*pieces), space(dim, rows), space(1, rows), space(*halves)]
    scratch += [space(dim, slots), space(*halves), one, *pairs(4), *total_spaces()]
    scratch += [*grads, space(dim, rels_pad), space(1, rels_pad)]
    scratch += [space(dim, slots), one, space(*pieces), *pairs(1), *total_spaces()]
    et, state, rt, rel_state = call(
        functools.partial(step_kernel, len(total_spaces())),
        [array(dim, rows), array(1, rows), array(dim, rels), array(1, rels_pad)],
        [
            entities.T,
            entity_state.reshape(1, rows),
            relations.T,
            jnp.pad(relation_state, (0, rels_pad - rels), constant_values=1.0).reshape(1, rels_pad),
            edges.transpose(1, 0, 2),
            negatives,
            counts.T,
        ],
        scratch,
        name="step",
        collective=0,
    )
    return et.T, state.reshape(rows), rt.T, rel_state[0, :rels]


def solution(mesh):
    return jax.shard_map(
        body,
        mesh=mesh,
        in_specs=(
            P("dom", None),
            P("dom"),
            P(),
            P(),
            P(None, None, "dom"),
            P(None, "dom", None),
            P(None, "dom"),
        ),
        out_specs=(P("dom", None), P("dom"), P(), P()),
        check_vma=False,
    )
```

```python
import functools

import jax
import jax.numpy as jnp
from jax import lax
from jax.experimental import pallas as pl
from jax.experimental.pallas import tpu as pltpu
from jax.sharding import PartitionSpec as P

RATE = 0.2
F32 = jnp.float32
BF16 = jnp.bfloat16
VMEM = pl.BlockSpec(memory_space=pltpu.VMEM)
SMEM = pl.BlockSpec(memory_space=pltpu.SMEM)
NN = (((1,), (0,)), ((), ()))
NT = (((1,), (1,)), ((), ()))
LANES = 128
SUBLANES = 8
ZS, XS, YS, CORES = 8, 4, 4, 2
PLANE = XS * YS
MESH = pl.DeviceIdType.MESH


def ring(apart, count):
    return min(apart, count - apart)


BY_DEPTH = sorted(range(1, ZS), key=lambda k: -ring(k, ZS))
BY_REACH = sorted(range(PLANE), key=lambda k: -ring(k // YS, XS) - ring(k % YS, YS))


def split(value):
    high = value.astype(BF16)
    return high, (value - high.astype(F32)).astype(BF16)


def dot(left, right, dims=NN):
    return lax.dot_general(left, right, dims, preferred_element_type=F32)


def dot3(left, right, dims=NN):
    return (
        dot(left[0], right[0], dims) + dot(left[0], right[1], dims) + dot(left[1], right[0], dims)
    )


def dot_exact(left, right, dims=NN):
    return dot(left[0], right, dims) + dot(left[1], right, dims)


def spots(ids, count):
    rows = lax.broadcasted_iota(jnp.int32, (count, ids.shape[1]), 0)
    return jnp.where(rows == ids, 1.0, 0.0).astype(BF16)


def call(kernel, outs, args, scratch=(), name=None, collective=None):
    params = None
    if collective is not None:
        params = pltpu.CompilerParams(collective_id=collective, has_side_effects=True)
    return pl.pallas_call(
        kernel,
        out_shape=[jax.ShapeDtypeStruct(*out) for out in outs],
        in_specs=[VMEM] * len(args),
        out_specs=[VMEM] * len(outs),
        scratch_shapes=list(scratch),
        compiler_params=params,
        name=name,
    )(*args)


def pairs(*counts):
    return [pltpu.SemaphoreType.DMA((count,)) for count in counts for _ in range(2)]


def hist(meta_ref, c_ref, blocks, draws):
    ones = jnp.ones((meta_ref.shape[1], LANES), BF16)
    for b in range(blocks):
        hits = spots(meta_ref[4 + b : 5 + b, :], c_ref.shape[0])
        c_ref[:, b * LANES : (b + 1) * LANES] = dot(hits, ones) * (1.0 / draws)


def table_parts(et_ref, wide, e_parts, et_parts):
    dim = et_ref.shape[0]
    wide[0:dim, :] = et_ref[...]
    wide[dim:, :] = jnp.zeros((wide.shape[0] - dim, wide.shape[1]), F32)
    e_parts[0][...], e_parts[1][...] = split(wide[...].T)
    et_parts[0][...], et_parts[1][...] = split(et_ref[...])


def relation_rows(rt_ref, meta_ref, picks, w):
    picks[...] = spots(meta_ref[1:2, 0 : w.shape[1]], rt_ref.shape[1])
    w[...] = dot_exact(split(rt_ref[...]), picks[...])


def edge_part(part, e_parts, et_parts, st, meta_ref, c_ref, picks, w, gt_ref, gs_ref, h_sum, q, tmp):
    dim, rows = et_parts[0].shape
    half = dim // 2
    wide = st.shape[1]
    lanes = slice(part * wide, (part + 1) * wide)
    number = lax.broadcasted_iota(jnp.int32, (1, wide), 1) + part * wide
    live = number < meta_ref[3:4, lanes]
    target = jnp.where(live, meta_ref[2:3, lanes], -1)
    alive = live.astype(F32)
    s_re, s_im = st[0:half, :], st[half:dim, :]
    w_re, w_im = w[0:half, lanes], w[half:dim, lanes]
    q[0:half, :] = s_re * w_re - s_im * w_im
    q[half:dim, :] = s_re * w_im + s_im * w_re
    q_parts = split(q[...])
    up = jnp.zeros((dim, wide), F32)
    step = 256
    for j in range(0, rows, step):
        e_part = [one[j : j + step, 0:dim] for one in e_parts]
        scores = dot3(e_part, q_parts)
        sig = 0.5 * jnp.tanh(0.5 * scores) + 0.5
        row = lax.broadcasted_iota(jnp.int32, (step, wide), 0) + j
        mark = jnp.where(row == target, 1.0, 0.0)
        weight = split(sig * (c_ref[j : j + step, lanes] * alive + mark) - mark)
        up = up + dot3([one[:, j : j + step] for one in et_parts], weight)
        grad = dot3(q_parts, weight, NT)
        gt_ref[:, j : j + step] = grad if part == 0 else gt_ref[:, j : j + step] + grad
    q[...] = up
    u_re, u_im = q[0:half, :], q[half:dim, :]
    gs_ref[0:half, lanes] = u_re * w_re + u_im * w_im
    gs_ref[half:dim, lanes] = u_im * w_re - u_re * w_im
    tmp[0:half, :] = u_re * s_re + u_im * s_im
    tmp[half:dim, :] = u_im * s_re - u_re * s_im
    total = dot_exact(split(tmp[...]), picks[:, lanes], NT)
    h_sum[...] = total if part == 0 else h_sum[...] + total


def cut_tiles(h_sum, h_ref):
    places, tiles = tile_places(h_ref.shape, h_sum.shape)
    for place, (row, lane) in zip(places, tiles):
        h_ref[place] = h_sum[row : row + SUBLANES, lane : lane + LANES]
    for place in places[len(tiles) :]:
        h_ref[place] = jnp.zeros((SUBLANES, LANES), F32)


def front(
    everyone, et_ref, r_ref, edges_ref, neg_ref, counts_ref,
    gt_ref, gs_ref, h_ref, rt_ref, meta_ref, meta1_ref, c1_ref,
    meta0, c0, st, rows, wide, eh, el, eth, etl, picks, w, h_sum, q, tmp, ss, rs,
):
    dim, count = et_ref.shape
    kinds, rounds, slots = edges_ref.shape
    blocks, draws = neg_ref.shape[1:]
    parts, _, width = st.shape
    c, y, x, z = places_of()
    far, near = device((z + ZS // 2) % ZS, x, y, c), other_core()
    greet(everyone)
    eth[...], etl[...] = split(et_ref[...])
    meta_ref[...] = jnp.full(meta_ref.shape, -1, jnp.int32)
    for r in range(rounds):
        for kind in range(kinds):
            meta_ref[r, kind : kind + 1, 0:slots] = edges_ref[kind, r : r + 1, :]
        meta_ref[r, kinds : kinds + 1, :] = jnp.broadcast_to(counts_ref[0:1, r : r + 1], (1, count))
        meta_ref[r, kinds + 1 : kinds + 1 + blocks, 0:draws] = neg_ref[r]
    sends = [remote(st.at[p], rows.at[p], (ss, rs), p, far) for p in range(parts)]
    sends.append(remote(meta_ref.at[0], meta0, (ss, rs), parts, far))
    sends.append(remote(meta_ref.at[1], meta1_ref, (ss, rs), parts + 1, near))
    for p in range(parts):
        source = meta_ref[0, 0:1, p * width : (p + 1) * width]
        st[p] = dot_exact((eth[...], etl[...]), spots(source, count))
        if p == 0:
            await_peers(everyone)
            sends[parts].start()
            sends[parts + 1].start()
        sends[p].start()
    wide[0:dim, :] = et_ref[...]
    wide[dim:, :] = jnp.zeros((wide.shape[0] - dim, count), F32)
    eh[...], el[...] = split(wide[...].T)
    rt_ref[...] = jnp.zeros_like(rt_ref)
    rt_ref[:, 0 : r_ref.shape[1]] = r_ref[...]
    sends[parts + 1].wait_recv()
    hist(meta1_ref, c1_ref, blocks, draws)
    sends[parts].wait_recv()
    hist(meta0, c0, blocks, draws)
    relation_rows(rt_ref, meta0, picks, w)
    for p in range(parts):
        sends[p].wait_recv()
        edge_part(
            p, (eh, el), (eth, etl), rows.at[p], meta0, c0, picks, w, gt_ref, gs_ref, h_sum, q, tmp
        )
    cut_tiles(h_sum, h_ref)
    for one in sends:
        one.wait_send()


def second_main(
    et_ref, rt_ref, rel_state_ref, sum_ref, rows, meta_ref, c_ref,
    gt_ref, gs_ref, h_ref, rt_out, rel_state_out,
    wide, eh, el, eth, etl, picks, w, h_sum, q, tmp,
):
    join_tiles(sum_ref, h_sum)
    rt_out[...], rel_state_out[...] = stepped(rt_ref[...], rel_state_ref[...], h_sum[...])
    table_parts(et_ref, wide, (eh, el), (eth, etl))
    relation_rows(rt_out, meta_ref, picks, w)
    for p in range(rows.shape[0]):
        edge_part(
            p, (eh, el), (eth, etl), rows.at[p], meta_ref, c_ref, picks, w, gt_ref, gs_ref, h_sum, q, tmp
        )
    cut_tiles(h_sum, h_ref)


def tile_places(shape, flat):
    places = [(c, k, t) for c in range(shape[0]) for k in range(shape[1]) for t in range(shape[2])]
    tiles = [(r, l) for r in range(0, flat[0], SUBLANES) for l in range(0, flat[1], LANES)]
    return places, tiles


def join_tiles(h_ref, whole):
    places, tiles = tile_places(h_ref.shape, whole.shape)
    for place, (row, lane) in zip(places, tiles):
        whole[row : row + SUBLANES, lane : lane + LANES] = h_ref[place]


def places_of():
    me = lax.axis_index("dom")
    return me % CORES, me // CORES % YS, me // (CORES * YS) % XS, me // (CORES * YS * XS)


def device(z, x, y, c):
    return (((z * XS + x) * YS + y) * CORES + c,)


def remote(src, dst, sems, k, to):
    return pltpu.make_async_remote_copy(
        src_ref=src,
        dst_ref=dst,
        send_sem=sems[0].at[k],
        recv_sem=sems[1].at[k],
        device_id=to,
        device_id_type=MESH,
    )


def greet(peers):
    for peer in peers:
        pl.semaphore_signal(
            pltpu.get_barrier_semaphore(), inc=1, device_id=peer, device_id_type=MESH
        )


def await_peers(peers):
    pl.semaphore_wait(pltpu.get_barrier_semaphore(), len(peers))


def other_core():
    c, y, x, z = places_of()
    return device(z, x, y, 1 - c)


def in_plane():
    c, y, x, z = places_of()
    plane = []
    for k in range(PLANE):
        px, py = (x + k // YS) % XS, (y + k % YS) % YS
        fx, fy = (x + XS - k // YS) % XS, (y + YS - k % YS) % YS
        plane.append((device(z, px, py, c), px * YS + py, fx * YS + fy))
    return plane


def in_column():
    c, y, x, z = places_of()
    return [device((z + k) % ZS, x, y, c) for k in range(ZS)]


def spread_sum(h_ref, out_ref, *more, beside=()):
    s0, r0, s1, r1 = more[-4:]
    acc, got0, got1 = (more[i * PLANE : (i + 1) * PLANE] for i in range(3))
    other = other_core()
    plane = in_plane()
    c = places_of()[0]
    order = BY_REACH
    first = [remote(h_ref.at[1 - c, plane[k][1]], got0[k], (s0, r0), k, other) for k in range(PLANE)]
    second = [None] + [remote(acc[k], got1[k], (s1, r1), k, plane[k][0]) for k in range(1, PLANE)]
    for k in order:
        first[k].start()
    for one in beside:
        one.start()
    last = 0
    for k in order:
        first[k].wait_recv()
        acc[k][...] = h_ref[c, plane[k][1]] + got0[k][...]
        if last:
            second[last].start()
        last = k
    total = acc[0][...]
    for k in order[:-1]:
        second[k].wait_recv()
        total = total + got1[k][...]
    out_ref[...] = total
    for one in first + second[1:]:
        one.wait_send()


def spread_column(
    h_ref, out_ref, level, part, own, s2, r2, s5, r5, *more, early=(), middle=(), late=(), during=None
):
    pair, got2, got5 = (more[i * ZS : (i + 1) * ZS] for i in range(3))
    more = more[3 * ZS :]
    z = places_of()[3]
    column = in_column()
    each = own.shape[0]
    spread_sum(h_ref, part, *more, beside=early)
    for k in range(ZS):
        pair[k][0:each] = part[pl.ds((z + k) % ZS * each, each)]
        pair[k][each:] = part[ZS * each :]
    third = [None] + [remote(pair[k], got2[k], (s2, r2), k, column[k]) for k in range(1, ZS)]
    for k in BY_DEPTH:
        third[k].start()
    for one in middle:
        one.start()
    level[z] = pair[0][...]
    for k in BY_DEPTH:
        third[k].wait_recv()
        level[(z + ZS - k) % ZS] = got2[k][...]
    total = level[0]
    for k in range(1, ZS):
        total = total + level[k]
    own[...] = total[0:each]
    given = [None] + [remote(own, got5[k], (s5, r5), k, column[k]) for k in range(1, ZS)]
    for k in BY_DEPTH:
        given[k].start()
    for one in late:
        one.start()
    out_ref[ZS * each :] = total[each:]
    out_ref[pl.ds(z * each, each)] = total[0:each]
    if during is not None:
        during()
    for k in BY_DEPTH:
        given[k].wait_recv()
        out_ref[pl.ds((z + ZS - k) % ZS * each, each)] = got5[k][...]
    for one in third[1:] + given[1:]:
        one.wait_send()


def spread_share(h_ref, out_ref, *more, beside=None):
    s3, r3, s4, r4 = more[-4:]
    got3, got4 = (more[i * PLANE : (i + 1) * PLANE] for i in range(2))
    other = other_core()
    plane = in_plane()
    c = places_of()[0]
    order = BY_REACH[:-1]
    fourth = [None] + [remote(h_ref, got3[k], (s3, r3), k, plane[k][0]) for k in range(1, PLANE)]
    fifth = [remote(got3[k] if k else h_ref, got4[k], (s4, r4), k, other) for k in range(PLANE)]
    for k in order:
        fourth[k].start()
    fifth[0].start()
    out_ref[c, plane[0][1]] = h_ref[...]
    for k in order:
        fourth[k].wait_recv()
        fifth[k].start()
        out_ref[c, plane[k][2]] = got3[k][...]
    if beside is not None:
        beside()
    for k in [0, *order]:
        fifth[k].wait_recv()
        out_ref[1 - c, plane[k][2]] = got4[k][...]
    for one in fourth[1:] + fifth:
        one.wait_send()


def first_total(
    h_ref, et_ref, state_ref, gt_ref, gs_ref, meta_ref,
    sums_ref, et_out, state_out, rows_out,
    gs_in, mine, both, sx, rx, *more,
):
    c, y, x, z = places_of()
    far = device((z + ZS // 2) % ZS, x, y, c)
    dim = gs_ref.shape[0]
    parts, _, width = mine.shape
    cuts = [dim * share // 100 // SUBLANES * SUBLANES for share in (0, 45, 70)] + [dim]
    ends = list(zip(cuts[:-1], cuts[1:]))
    back = [remote(gs_ref.at[a:b], gs_in.at[a:b], (sx, rx), i, far) for i, (a, b) in enumerate(ends)]
    on = [remote(mine.at[p], rows_out.at[p], (sx, rx), 3 + p, other_core()) for p in range(parts)]
    more, share = more[: -2 * PLANE - 4], more[-2 * PLANE - 4 :]
    spread_column(h_ref, both, *more, early=back[:1], middle=back[1:2], late=back[2:])

    def beside():
        for one in back:
            one.wait()
        after = entity_step(0, et_ref, state_ref, gt_ref, gs_in, meta_ref, state_out)
        et_out[...] = after
        pieces = split(after)
        for p in range(parts):
            source = meta_ref[1, 0:1, p * width : (p + 1) * width]
            mine[p] = dot_exact(pieces, spots(source, after.shape[1]))
            on[p].start()

    spread_share(both, sums_ref, *share, beside=beside)
    for one in on:
        one.wait()


def last_total(
    h_ref, et_ref, state_ref, gt_ref, gs_ref, meta_ref, rt_ref, rel_state_ref,
    et_out, state_out, rt_out, rel_state_out,
    gs_in, both, sums, whole, sx, rx, *more,
):
    near = remote(gs_ref, gs_in, (sx, rx), 0, other_core())

    def during():
        near.wait()
        et_out[...] = entity_step(1, et_ref, state_ref, gt_ref, gs_in, meta_ref, state_out)

    more, share = more[: -2 * PLANE - 4], more[-2 * PLANE - 4 :]
    spread_column(h_ref, both, *more, early=[near], during=during)
    spread_share(both, sums, *share)
    join_tiles(sums, whole)
    after, state = stepped(rt_ref[...], rel_state_ref[...], whole[...])
    rt_out[...] = after[:, 0 : rt_out.shape[1]]
    rel_state_out[...] = state


def step_kernel(sizes, *refs):
    refs = list(refs)

    def take(count):
        taken, refs[:count] = refs[:count], []
        return taken

    et, state, r, rel_state_flat, edges, neg, counts = take(7)
    et_out, state_out, rt_out, rel_state_out = take(4)
    gt, gs, h, rt, meta, meta1, c1, meta0, c0, st, rows = take(11)
    table = take(10)
    front_sems = take(2)
    sums, et1, state1, their_rows, gs_in, mine, both, sx, rx = take(9)
    first_spaces = take(sizes)
    gt1, gs1, h1, rt1, rel_state1, rel_state = take(6)
    gs_in1, both1, sums1, sx1, rx1 = take(5)
    last_spaces = take(sizes)
    everyone = [other_core()] + [one[0] for one in in_plane()[1:]] + in_column()[1:]
    front(
        everyone, et, r, edges, neg, counts, gt, gs, h, rt, meta, meta1, c1, meta0, c0, st, rows,
        *table, *front_sems,
    )
    first_total(
        h, et, state, gt, gs, meta, sums, et1, state1, their_rows, gs_in, mine, both, sx, rx,
        *first_spaces,
    )
    rel_state[...] = jnp.ones_like(rel_state)
    rel_state[0, 0 : rel_state_flat.shape[0]] = rel_state_flat[...]
    second_main(
        et1, rt, rel_state, sums, their_rows, meta1, c1, gt1, gs1, h1, rt1, rel_state1, *table
    )
    last_total(
        h1, et1, state1, gt1, gs1, meta, rt1, rel_state1, et_out, state_out, rt_out, rel_state_out,
        gs_in1, both1, sums1, table[7], sx1, rx1, *last_spaces,
    )


def finish_kernel(et_ref, state_ref, rt_ref, rel_state_ref, et_out, state_out, rt_out, rel_state_out):
    et_out[...] = et_ref[...]
    rt_out[...] = rt_ref[...]
    state_out[...] = state_ref[0]
    rel_state_out[...] = rel_state_ref[0, 0 : rel_state_out.shape[0]]


def entity_step(number, et_ref, state_ref, gt_ref, gs_ref, meta_ref, state_out):
    source = spots(meta_ref[number, 0:1, 0 : gs_ref.shape[1]], et_ref.shape[1])
    grad = gt_ref[...] + dot_exact(split(gs_ref[...]), source, NT)
    after, state_out[...] = stepped(et_ref[...], state_ref[...], grad)
    return after


def stepped(param, state, grad):
    new_state = state + jnp.sum(grad * grad, axis=0, keepdims=True) * (1.0 / grad.shape[0])
    return param - RATE * grad / jnp.sqrt(new_state), new_state


def body(entities, entity_state, relations, relation_state, edges, negatives, counts):
    rows, dim = entities.shape
    rels = relations.shape[0]
    rels_pad = -(-rels // LANES) * LANES
    slots = edges.shape[2]
    blocks, draws = negatives.shape[1:]
    dim_pad = -(-dim // LANES) * LANES
    tiles = dim // SUBLANES * (rels_pad // LANES)
    piece = (-(-tiles // (CORES * PLANE)), SUBLANES, LANES)
    pieces = (CORES, PLANE, *piece)
    halves = (2, dim, slots // 2)
    each = piece[0] // ZS
    pair = (piece[0] - (ZS - 1) * each, SUBLANES, LANES)
    one, own = pltpu.VMEM(piece, F32), pltpu.VMEM((each, SUBLANES, LANES), F32)

    def array(*shape, kind=F32):
        return (shape, kind)

    def space(*shape, kind=F32):
        return pltpu.VMEM(shape, kind)

    def table_spaces():
        return [
            space(dim_pad, rows),
            space(rows, dim_pad, kind=BF16),
            space(rows, dim_pad, kind=BF16),
            space(dim, rows, kind=BF16),
            space(dim, rows, kind=BF16),
            space(rels_pad, slots, kind=BF16),
            space(dim, slots),
            space(dim, rels_pad),
            space(*halves[1:]),
            space(*halves[1:]),
        ]

    def total_spaces():
        return (
            [space(ZS, *pair), one, own, *pairs(ZS, ZS)]
            + [space(*pair)] * (2 * ZS)
            + [own] * ZS
            + [one] * (3 * PLANE)
            + pairs(PLANE, PLANE)
            + [one] * (2 * PLANE)
            + pairs(PLANE, PLANE)
        )

    meta_shape = (2, 4 + blocks, rows)
    meta = space(*meta_shape, kind=jnp.int32)
    one_meta = space(*meta_shape[1:], kind=jnp.int32)
    grads = [space(dim, rows), space(dim, slots), space(*pieces)]
    scratch = [*grads, space(dim, rels_pad), meta, one_meta, space(rows, slots), one_meta]
    scratch += [space(rows, slots), space(*halves), space(*halves), *table_spaces(), *pairs(4)]
    scratch += [space(*pieces), space(dim, rows), space(1, rows), space(*halves)]
    scratch += [space(dim, slots), space(*halves), one, *pairs(5), *total_spaces()]
    scratch += [*grads, space(dim, rels_pad), space(1, rels_pad), space(1, rels_pad)]
    scratch += [space(dim, slots), one, space(*pieces), *pairs(1), *total_spaces()]
    et, state, rt, rel_state = call(
        functools.partial(step_kernel, len(total_spaces())),
        [array(dim, rows), array(1, rows), array(dim, rels), array(1, rels_pad)],
        [
            entities.T,
            entity_state.reshape(1, rows),
            relations.T,
            relation_state,
            edges.transpose(1, 0, 2),
            negatives,
            counts.T,
        ],
        scratch,
        name="step",
        collective=0,
    )
    et, state, rt, rel_state = call(
        finish_kernel,
        [array(dim, rows), array(rows), array(dim, rels), array(rels)],
        [et, state, rt, rel_state],
        name="finish",
    )
    return et.T, state, rt.T, rel_state


def solution(mesh):
    return jax.shard_map(
        body,
        mesh=mesh,
        in_specs=(
            P("dom", None),
            P("dom"),
            P(),
            P(),
            P(None, None, "dom"),
            P(None, "dom", None),
            P(None, "dom"),
        ),
        out_specs=(P("dom", None), P("dom"), P(), P()),
        check_vma=False,
    )
```

```python
import functools

import jax
import jax.numpy as jnp
from jax import lax
from jax.experimental import pallas as pl
from jax.experimental.pallas import tpu as pltpu
from jax.sharding import PartitionSpec as P

RATE = 0.2
F32 = jnp.float32
BF16 = jnp.bfloat16
VMEM = pl.BlockSpec(memory_space=pltpu.VMEM)
SMEM = pl.BlockSpec(memory_space=pltpu.SMEM)
NN = (((1,), (0,)), ((), ()))
NT = (((1,), (1,)), ((), ()))
LANES = 128
SUBLANES = 8
ZS, XS, YS, CORES = 8, 4, 4, 2
PLANE = XS * YS
MESH = pl.DeviceIdType.MESH


def ring(apart, count):
    return min(apart, count - apart)


BY_DEPTH = sorted(range(1, ZS), key=lambda k: -ring(k, ZS))
BY_REACH = sorted(range(PLANE), key=lambda k: -ring(k // YS, XS) - ring(k % YS, YS))


def split(value):
    high = value.astype(BF16)
    return high, (value - high.astype(F32)).astype(BF16)


def dot(left, right, dims=NN):
    return lax.dot_general(left, right, dims, preferred_element_type=F32)


def dot3(left, right, dims=NN):
    return (
        dot(left[0], right[0], dims) + dot(left[0], right[1], dims) + dot(left[1], right[0], dims)
    )


def dot_exact(left, right, dims=NN):
    return dot(left[0], right, dims) + dot(left[1], right, dims)


def spots(ids, count):
    rows = lax.broadcasted_iota(jnp.int32, (count, ids.shape[1]), 0)
    return jnp.where(rows == ids, 1.0, 0.0).astype(BF16)


def call(kernel, outs, args, scratch=(), name=None, collective=None):
    params = None
    if collective is not None:
        params = pltpu.CompilerParams(collective_id=collective, has_side_effects=True)
    return pl.pallas_call(
        kernel,
        out_shape=[jax.ShapeDtypeStruct(*out) for out in outs],
        in_specs=[VMEM] * len(args),
        out_specs=[VMEM] * len(outs),
        scratch_shapes=list(scratch),
        compiler_params=params,
        name=name,
    )(*args)


def pairs(*counts):
    return [pltpu.SemaphoreType.DMA((count,)) for count in counts for _ in range(2)]


def hist(meta_ref, c_ref, blocks, draws):
    ones = jnp.ones((meta_ref.shape[1], LANES), BF16)
    for b in range(blocks):
        hits = spots(meta_ref[4 + b : 5 + b, :], c_ref.shape[0])
        c_ref[:, b * LANES : (b + 1) * LANES] = dot(hits, ones) * (1.0 / draws)


def table_parts(et_ref, wide, e_parts, et_parts):
    dim = et_ref.shape[0]
    wide[0:dim, :] = et_ref[...]
    wide[dim:, :] = jnp.zeros((wide.shape[0] - dim, wide.shape[1]), F32)
    e_parts[0][...], e_parts[1][...] = split(wide[...].T)
    et_parts[0][...], et_parts[1][...] = split(et_ref[...])


def relation_rows(rt_ref, meta_ref, picks, w):
    picks[...] = spots(meta_ref[1:2, 0 : w.shape[1]], rt_ref.shape[1])
    w[...] = dot_exact(split(rt_ref[...]), picks[...])


def edge_part(part, e_parts, et_parts, st, meta_ref, c_ref, picks, w, gt_ref, gs_ref, h_sum, q, tmp):
    dim, rows = et_parts[0].shape
    half = dim // 2
    wide = st.shape[1]
    lanes = slice(part * wide, (part + 1) * wide)
    number = lax.broadcasted_iota(jnp.int32, (1, wide), 1) + part * wide
    live = number < meta_ref[3:4, lanes]
    target = jnp.where(live, meta_ref[2:3, lanes], -1)
    alive = live.astype(F32)
    s_re, s_im = st[0:half, :], st[half:dim, :]
    w_re, w_im = w[0:half, lanes], w[half:dim, lanes]
    q[0:half, :] = s_re * w_re - s_im * w_im
    q[half:dim, :] = s_re * w_im + s_im * w_re
    q_parts = split(q[...])
    up = jnp.zeros((dim, wide), F32)
    step = 256
    for j in range(0, rows, step):
        e_part = [one[j : j + step, 0:dim] for one in e_parts]
        scores = dot3(e_part, q_parts)
        sig = 0.5 * jnp.tanh(0.5 * scores) + 0.5
        row = lax.broadcasted_iota(jnp.int32, (step, wide), 0) + j
        mark = jnp.where(row == target, 1.0, 0.0)
        weight = split(sig * (c_ref[j : j + step, lanes] * alive + mark) - mark)
        up = up + dot3([one[:, j : j + step] for one in et_parts], weight)
        grad = dot3(q_parts, weight, NT)
        gt_ref[:, j : j + step] = grad if part == 0 else gt_ref[:, j : j + step] + grad
    q[...] = up
    u_re, u_im = q[0:half, :], q[half:dim, :]
    gs_ref[0:half, lanes] = u_re * w_re + u_im * w_im
    gs_ref[half:dim, lanes] = u_im * w_re - u_re * w_im
    tmp[0:half, :] = u_re * s_re + u_im * s_im
    tmp[half:dim, :] = u_im * s_re - u_re * s_im
    total = dot_exact(split(tmp[...]), picks[:, lanes], NT)
    h_sum[...] = total if part == 0 else h_sum[...] + total


def cut_tiles(h_sum, h_ref):
    places, tiles = tile_places(h_ref.shape, h_sum.shape)
    for place, (row, lane) in zip(places, tiles):
        h_ref[place] = h_sum[row : row + SUBLANES, lane : lane + LANES]
    for place in places[len(tiles) :]:
        h_ref[place] = jnp.zeros((SUBLANES, LANES), F32)


def front(
    everyone, et_ref, r_ref, edges_ref, neg_ref, counts_ref,
    gt_ref, gs_ref, h_ref, rt_ref, meta_ref, meta1_ref, c1_ref,
    meta0, c0, st, rows, wide, eh, el, eth, etl, picks, w, h_sum, q, tmp, ss, rs,
):
    dim, count = et_ref.shape
    kinds, rounds, slots = edges_ref.shape
    blocks, draws = neg_ref.shape[1:]
    parts, _, width = st.shape
    c, y, x, z = places_of()
    far, near = device((z + ZS // 2) % ZS, x, y, c), other_core()
    greet(everyone)
    eth[...], etl[...] = split(et_ref[...])
    meta_ref[...] = jnp.full(meta_ref.shape, -1, jnp.int32)
    for r in range(rounds):
        for kind in range(kinds):
            meta_ref[r, kind : kind + 1, 0:slots] = edges_ref[kind, r : r + 1, :]
        meta_ref[r, kinds : kinds + 1, :] = jnp.broadcast_to(counts_ref[0:1, r : r + 1], (1, count))
        meta_ref[r, kinds + 1 : kinds + 1 + blocks, 0:draws] = neg_ref[r]
    sends = [remote(st.at[p], rows.at[p], (ss, rs), p, far) for p in range(parts)]
    sends.append(remote(meta_ref.at[0], meta0, (ss, rs), parts, far))
    sends.append(remote(meta_ref.at[1], meta1_ref, (ss, rs), parts + 1, near))
    for p in range(parts):
        source = meta_ref[0, 0:1, p * width : (p + 1) * width]
        st[p] = dot_exact((eth[...], etl[...]), spots(source, count))
        if p == 0:
            await_peers(everyone)
            sends[parts].start()
            sends[parts + 1].start()
        sends[p].start()
    wide[0:dim, :] = et_ref[...]
    wide[dim:, :] = jnp.zeros((wide.shape[0] - dim, count), F32)
    eh[...], el[...] = split(wide[...].T)
    rt_ref[...] = jnp.zeros_like(rt_ref)
    rt_ref[:, 0 : r_ref.shape[1]] = r_ref[...]
    sends[parts + 1].wait_recv()
    hist(meta1_ref, c1_ref, blocks, draws)
    sends[parts].wait_recv()
    hist(meta0, c0, blocks, draws)
    relation_rows(rt_ref, meta0, picks, w)
    for p in range(parts):
        sends[p].wait_recv()
        edge_part(
            p, (eh, el), (eth, etl), rows.at[p], meta0, c0, picks, w, gt_ref, gs_ref, h_sum, q, tmp
        )
    cut_tiles(h_sum, h_ref)
    for one in sends:
        one.wait_send()


def second_main(
    et_ref, rt_ref, rel_state_ref, sum_ref, rows, meta_ref, c_ref,
    gt_ref, gs_ref, h_ref, rt_out, rel_state_out,
    arriving, wide, eh, el, eth, etl, picks, w, h_sum, q, tmp,
):
    join_tiles(sum_ref, h_sum)
    rt_out[...], rel_state_out[...] = stepped(rt_ref[...], rel_state_ref[...], h_sum[...])
    relation_rows(rt_out, meta_ref, picks, w)
    for p in range(rows.shape[0]):
        arriving[p].wait_recv()
        edge_part(
            p, (eh, el), (eth, etl), rows.at[p], meta_ref, c_ref, picks, w, gt_ref, gs_ref, h_sum, q, tmp
        )
    cut_tiles(h_sum, h_ref)


def tile_places(shape, flat):
    places = [(c, k, t) for c in range(shape[0]) for k in range(shape[1]) for t in range(shape[2])]
    tiles = [(r, l) for r in range(0, flat[0], SUBLANES) for l in range(0, flat[1], LANES)]
    return places, tiles


def join_tiles(h_ref, whole):
    places, tiles = tile_places(h_ref.shape, whole.shape)
    for place, (row, lane) in zip(places, tiles):
        whole[row : row + SUBLANES, lane : lane + LANES] = h_ref[place]


def places_of():
    me = lax.axis_index("dom")
    return me % CORES, me // CORES % YS, me // (CORES * YS) % XS, me // (CORES * YS * XS)


def device(z, x, y, c):
    return (((z * XS + x) * YS + y) * CORES + c,)


def remote(src, dst, sems, k, to):
    return pltpu.make_async_remote_copy(
        src_ref=src,
        dst_ref=dst,
        send_sem=sems[0].at[k],
        recv_sem=sems[1].at[k],
        device_id=to,
        device_id_type=MESH,
    )


def greet(peers):
    for peer in peers:
        pl.semaphore_signal(
            pltpu.get_barrier_semaphore(), inc=1, device_id=peer, device_id_type=MESH
        )


def await_peers(peers):
    pl.semaphore_wait(pltpu.get_barrier_semaphore(), len(peers))


def other_core():
    c, y, x, z = places_of()
    return device(z, x, y, 1 - c)


def in_plane():
    c, y, x, z = places_of()
    plane = []
    for k in range(PLANE):
        px, py = (x + k // YS) % XS, (y + k % YS) % YS
        fx, fy = (x + XS - k // YS) % XS, (y + YS - k % YS) % YS
        plane.append((device(z, px, py, c), px * YS + py, fx * YS + fy))
    return plane


def in_column():
    c, y, x, z = places_of()
    return [device((z + k) % ZS, x, y, c) for k in range(ZS)]


def spread_sum(h_ref, out_ref, *more, beside=()):
    s0, r0, s1, r1 = more[-4:]
    acc, got0, got1 = (more[i * PLANE : (i + 1) * PLANE] for i in range(3))
    other = other_core()
    plane = in_plane()
    c = places_of()[0]
    order = BY_REACH
    first = [remote(h_ref.at[1 - c, plane[k][1]], got0[k], (s0, r0), k, other) for k in range(PLANE)]
    second = [None] + [remote(acc[k], got1[k], (s1, r1), k, plane[k][0]) for k in range(1, PLANE)]
    for k in order:
        first[k].start()
    for one in beside:
        one.start()
    last = 0
    for k in order:
        first[k].wait_recv()
        acc[k][...] = h_ref[c, plane[k][1]] + got0[k][...]
        if last:
            second[last].start()
        last = k
    total = acc[0][...]
    for k in order[:-1]:
        second[k].wait_recv()
        total = total + got1[k][...]
    out_ref[...] = total
    for one in first + second[1:]:
        one.wait_send()


def spread_column(
    h_ref, out_ref, level, part, own, s2, r2, s5, r5, *more, early=(), middle=(), late=(), during=None
):
    pair, got2, got5 = (more[i * ZS : (i + 1) * ZS] for i in range(3))
    more = more[3 * ZS :]
    z = places_of()[3]
    column = in_column()
    each = own.shape[0]
    spread_sum(h_ref, part, *more, beside=early)
    for k in range(ZS):
        pair[k][0:each] = part[pl.ds((z + k) % ZS * each, each)]
        pair[k][each:] = part[ZS * each :]
    third = [None] + [remote(pair[k], got2[k], (s2, r2), k, column[k]) for k in range(1, ZS)]
    for k in BY_DEPTH:
        third[k].start()
    for one in middle:
        one.start()
    level[z] = pair[0][...]
    for k in BY_DEPTH:
        third[k].wait_recv()
        level[(z + ZS - k) % ZS] = got2[k][...]
    total = level[0]
    for k in range(1, ZS):
        total = total + level[k]
    own[...] = total[0:each]
    given = [None] + [remote(own, got5[k], (s5, r5), k, column[k]) for k in range(1, ZS)]
    for k in BY_DEPTH:
        given[k].start()
    for one in late:
        one.start()
    out_ref[ZS * each :] = total[each:]
    out_ref[pl.ds(z * each, each)] = total[0:each]
    if during is not None:
        during()
    for k in BY_DEPTH:
        given[k].wait_recv()
        out_ref[pl.ds((z + ZS - k) % ZS * each, each)] = got5[k][...]
    for one in third[1:] + given[1:]:
        one.wait_send()


def spread_share(h_ref, out_ref, *more, beside=None):
    s3, r3, s4, r4 = more[-4:]
    got3, got4 = (more[i * PLANE : (i + 1) * PLANE] for i in range(2))
    other = other_core()
    plane = in_plane()
    c = places_of()[0]
    order = BY_REACH[:-1]
    fourth = [None] + [remote(h_ref, got3[k], (s3, r3), k, plane[k][0]) for k in range(1, PLANE)]
    fifth = [remote(got3[k] if k else h_ref, got4[k], (s4, r4), k, other) for k in range(PLANE)]
    for k in order:
        fourth[k].start()
    fifth[0].start()
    out_ref[c, plane[0][1]] = h_ref[...]
    for k in order:
        fourth[k].wait_recv()
        fifth[k].start()
        out_ref[c, plane[k][2]] = got3[k][...]
    if beside is not None:
        beside()
    for k in [0, *order]:
        fifth[k].wait_recv()
        out_ref[1 - c, plane[k][2]] = got4[k][...]
    for one in fourth[1:] + fifth:
        one.wait_send()


def first_total(
    h_ref, et_ref, state_ref, gt_ref, gs_ref, meta_ref,
    sums_ref, et_out, state_out, rows_out,
    gs_in, mine, both, sx, rx, *more, prepare,
):
    c, y, x, z = places_of()
    far = device((z + ZS // 2) % ZS, x, y, c)
    dim = gs_ref.shape[0]
    parts, _, width = mine.shape
    cuts = [dim * share // 100 // SUBLANES * SUBLANES for share in (0, 55, 80)] + [dim]
    ends = list(zip(cuts[:-1], cuts[1:]))
    back = [remote(gs_ref.at[a:b], gs_in.at[a:b], (sx, rx), i, far) for i, (a, b) in enumerate(ends)]
    on = [remote(mine.at[p], rows_out.at[p], (sx, rx), 3 + p, other_core()) for p in range(parts)]
    more, share = more[: -2 * PLANE - 4], more[-2 * PLANE - 4 :]
    spread_column(h_ref, both, *more, early=back[:1], middle=back[1:2], late=back[2:])

    def beside():
        for one in back:
            one.wait()
        after = entity_step(0, et_ref, state_ref, gt_ref, gs_in, meta_ref, state_out)
        et_out[...] = after
        pieces = split(after)
        for p in range(parts):
            source = meta_ref[1, 0:1, p * width : (p + 1) * width]
            mine[p] = dot_exact(pieces, spots(source, after.shape[1]))
            on[p].start()

        prepare()

    spread_share(both, sums_ref, *share, beside=beside)
    return on


def last_total(
    h_ref, et_ref, state_ref, gt_ref, gs_ref, meta_ref, rt_ref, rel_state_ref,
    et_out, state_out, rt_out, rel_state_out,
    gs_in, both, sums, whole, sx, rx, *more,
):
    near = remote(gs_ref, gs_in, (sx, rx), 0, other_core())

    def during():
        near.wait()
        et_out[...] = entity_step(1, et_ref, state_ref, gt_ref, gs_in, meta_ref, state_out)

    more, share = more[: -2 * PLANE - 4], more[-2 * PLANE - 4 :]
    spread_column(h_ref, both, *more, early=[near], during=during)
    spread_share(both, sums, *share)
    join_tiles(sums, whole)
    after, state = stepped(rt_ref[...], rel_state_ref[...], whole[...])
    rt_out[...] = after[:, 0 : rt_out.shape[1]]
    rel_state_out[...] = state


def step_kernel(sizes, *refs):
    refs = list(refs)

    def take(count):
        taken, refs[:count] = refs[:count], []
        return taken

    et, state, r, rel_state_flat, edges, neg, counts = take(7)
    et_out, state_out, rt_out, rel_state_out = take(4)
    gt, gs, h, rt, meta, meta1, c1, meta0, c0, st, rows = take(11)
    table = take(10)
    front_sems = take(2)
    sums, et1, state1, their_rows, gs_in, mine, both, sx, rx = take(9)
    first_spaces = take(sizes)
    gt1, gs1, h1, rt1, rel_state1, rel_state = take(6)
    gs_in1, both1, sums1, sx1, rx1 = take(5)
    last_spaces = take(sizes)
    everyone = [other_core()] + [one[0] for one in in_plane()[1:]] + in_column()[1:]
    front(
        everyone, et, r, edges, neg, counts, gt, gs, h, rt, meta, meta1, c1, meta0, c0, st, rows,
        *table, *front_sems,
    )
    arriving = first_total(
        h, et, state, gt, gs, meta, sums, et1, state1, their_rows, gs_in, mine, both, sx, rx,
        *first_spaces,
        prepare=lambda: table_parts(et1, table[0], table[1:3], table[3:5]),
    )
    rel_state[...] = jnp.ones_like(rel_state)
    rel_state[0, 0 : rel_state_flat.shape[0]] = rel_state_flat[...]
    second_main(
        et1, rt, rel_state, sums, their_rows, meta1, c1, gt1, gs1, h1, rt1, rel_state1,
        arriving, *table,
    )
    for one in arriving:
        one.wait_send()
    last_total(
        h1, et1, state1, gt1, gs1, meta, rt1, rel_state1, et_out, state_out, rt_out, rel_state_out,
        gs_in1, both1, sums1, table[7], sx1, rx1, *last_spaces,
    )


def finish_kernel(et_ref, state_ref, rt_ref, rel_state_ref, et_out, state_out, rt_out, rel_state_out):
    et_out[...] = et_ref[...]
    rt_out[...] = rt_ref[...]
    state_out[...] = state_ref[0]
    rel_state_out[...] = rel_state_ref[0, 0 : rel_state_out.shape[0]]


def entity_step(number, et_ref, state_ref, gt_ref, gs_ref, meta_ref, state_out):
    source = spots(meta_ref[number, 0:1, 0 : gs_ref.shape[1]], et_ref.shape[1])
    grad = gt_ref[...] + dot_exact(split(gs_ref[...]), source, NT)
    after, state_out[...] = stepped(et_ref[...], state_ref[...], grad)
    return after


def stepped(param, state, grad):
    new_state = state + jnp.sum(grad * grad, axis=0, keepdims=True) * (1.0 / grad.shape[0])
    return param - RATE * grad / jnp.sqrt(new_state), new_state


def body(entities, entity_state, relations, relation_state, edges, negatives, counts):
    rows, dim = entities.shape
    rels = relations.shape[0]
    rels_pad = -(-rels // LANES) * LANES
    slots = edges.shape[2]
    blocks, draws = negatives.shape[1:]
    dim_pad = -(-dim // LANES) * LANES
    tiles = dim // SUBLANES * (rels_pad // LANES)
    piece = (-(-tiles // (CORES * PLANE)), SUBLANES, LANES)
    pieces = (CORES, PLANE, *piece)
    halves = (2, dim, slots // 2)
    each = piece[0] // ZS
    pair = (piece[0] - (ZS - 1) * each, SUBLANES, LANES)
    one, own = pltpu.VMEM(piece, F32), pltpu.VMEM((each, SUBLANES, LANES), F32)

    def array(*shape, kind=F32):
        return (shape, kind)

    def space(*shape, kind=F32):
        return pltpu.VMEM(shape, kind)

    def table_spaces():
        return [
            space(dim_pad, rows),
            space(rows, dim_pad, kind=BF16),
            space(rows, dim_pad, kind=BF16),
            space(dim, rows, kind=BF16),
            space(dim, rows, kind=BF16),
            space(rels_pad, slots, kind=BF16),
            space(dim, slots),
            space(dim, rels_pad),
            space(*halves[1:]),
            space(*halves[1:]),
        ]

    def total_spaces():
        return (
            [space(ZS, *pair), one, own, *pairs(ZS, ZS)]
            + [space(*pair)] * (2 * ZS)
            + [own] * ZS
            + [one] * (3 * PLANE)
            + pairs(PLANE, PLANE)
            + [one] * (2 * PLANE)
            + pairs(PLANE, PLANE)
        )

    meta_shape = (2, 4 + blocks, rows)
    meta = space(*meta_shape, kind=jnp.int32)
    one_meta = space(*meta_shape[1:], kind=jnp.int32)
    grads = [space(dim, rows), space(dim, slots), space(*pieces)]
    scratch = [*grads, space(dim, rels_pad), meta, one_meta, space(rows, slots), one_meta]
    scratch += [space(rows, slots), space(*halves), space(*halves), *table_spaces(), *pairs(4)]
    scratch += [space(*pieces), space(dim, rows), space(1, rows), space(*halves)]
    scratch += [space(dim, slots), space(*halves), one, *pairs(5), *total_spaces()]
    scratch += [*grads, space(dim, rels_pad), space(1, rels_pad), space(1, rels_pad)]
    scratch += [space(dim, slots), one, space(*pieces), *pairs(1), *total_spaces()]
    et, state, rt, rel_state = call(
        functools.partial(step_kernel, len(total_spaces())),
        [array(dim, rows), array(1, rows), array(dim, rels), array(1, rels_pad)],
        [
            entities.T,
            entity_state.reshape(1, rows),
            relations.T,
            relation_state,
            edges.transpose(1, 0, 2),
            negatives,
            counts.T,
        ],
        scratch,
        name="step",
        collective=0,
    )
    et, state, rt, rel_state = call(
        finish_kernel,
        [array(dim, rows), array(rows), array(dim, rels), array(rels)],
        [et, state, rt, rel_state],
        name="finish",
    )
    return et.T, state, rt.T, rel_state


def solution(mesh):
    return jax.shard_map(
        body,
        mesh=mesh,
        in_specs=(
            P("dom", None),
            P("dom"),
            P(),
            P(),
            P(None, None, "dom"),
            P(None, "dom", None),
            P(None, "dom"),
        ),
        out_specs=(P("dom", None), P("dom"), P(), P()),
        check_vma=False,
    )
```
